32 devices in a mesh: gx: 2 (over y), gy: 4 (over x, core), gz: 4 (over z).
Axes of the slice: x: 2, y: 2, z: 4, core: 2. Of those that a mesh axis runs over, the one named last changes fastest.
Arguments:
- volume: float32 [16, 64, 512], P(('gx', 'gy'), None, 'gz'), may hold values from 0 to 1
- levels: int32 [4], replicated, may hold values from 0 to 255
Outputs:
- labelling: float32 [4, 16, 64, 512], P(None, 'gx', 'gy', 'gz')
- centers: float32 [4], replicated
The draws below stay inside these ranges and needn't reach their ends.
All inputs are finite; a program needn't handle non-finite values.
Results may differ from the reference program's by a relative error of at most 0.0001.
Values sent between devices are 32-bit elements; how exact they have to be, the bound alone decides.
A program may use at most 64 MiB of HBM per device.

```python
import jax
import jax.numpy as jnp
from jax import lax

LABELS = 4
ITERS = 2
NX = 16
NY = 64
NZ = 512


def with_ends(result, key, least, high):
    longest = result.shape.index(max(result.shape))
    spots = []
    for shift in (0, 1):
        where = [jax.random.randint(jax.random.fold_in(key, axis), (), 0, length) for axis, length in enumerate(result.shape)]
        where[longest] = (where[longest] + shift) % result.shape[longest]
        spots.append(tuple(where))
    return result.at[spots[0]].set(least).at[spots[1]].set(high)


def steps_of(rng, shape, pieces, least, largest):
    level, own = 1.0, jax.random.fold_in(rng, 6)
    for dim, parts in pieces:
        draws = jnp.exp(jax.random.uniform(jax.random.fold_in(own, dim), (parts,), jnp.float32, least / len(pieces), largest / len(pieces)))
        level = level * jnp.repeat(draws, shape[dim] // parts).reshape([-1 if axis == dim else 1 for axis in range(len(shape))])
    return level


def setup_inputs(seed: int = 0) -> dict:
    key_of = jax.random.split(jax.random.key(seed), 3)
    return {
        "volume": jnp.clip(1.0 * jax.random.uniform(key_of[0], (NX, NY, NZ), jnp.float32) ** steps_of(key_of[0], (NX, NY, NZ), ((0, 8), (2, 4)), -0.2, 0.2), 0.0, 1.0),
        "levels": with_ends(jax.random.randint(key_of[1], (LABELS,), 0, 256), jax.random.fold_in(key_of[1], 1), 0, 255).astype(jnp.int32),
    }


tau_step = 0.25
sigma_step = 0.25
smooth_weight = 0.5
prior_weight = 1.0

def project_simplex(values):
    how_many = values.shape[0]
    threshold = None
    for subset in range(1, 1 << how_many):
        members = [label_index for label_index in range(how_many) if subset >> label_index & 1]
        summed = values[members[0]]
        for label_index in members[1:]:
            summed = summed + values[label_index]
        candidate = (summed - 1.0) / float(len(members))
        threshold = candidate if threshold is None else jnp.maximum(threshold, candidate)
    return jnp.maximum(values - threshold[None], 0.0)

def forward(values, axis):
    extent = values.shape[axis]
    return jnp.diff(values, axis=axis, append=lax.slice_in_dim(values, extent - 1, extent, axis=axis))

def backward(values, axis):
    return jnp.diff(values, axis=axis, prepend=jnp.float32(0.0))

def reference(volume, levels):
    base_levels = levels.astype(jnp.float32) / 255.0
    centers = base_levels
    starting = (volume[None] - base_levels[:, None, None, None]) ** 2
    labelling = project_simplex(1.0 / LABELS - tau_step * starting)
    smoothed = labelling
    dual_field = [[jnp.zeros((NX, NY, NZ), jnp.float32) for axis in range(3)] for label_index in range(LABELS)]
    for iteration in range(ITERS):
        divergences = []
        renewed = []
        for label_index in range(LABELS):
            stepped = [dual_field[label_index][axis] + sigma_step * forward(smoothed[label_index], axis) for axis in range(3)]
            length = jnp.sqrt(stepped[0] * stepped[0] + stepped[1] * stepped[1] + stepped[2] * stepped[2])
            shrink = 1.0 / jnp.maximum(1.0, length / smooth_weight)
            projected = [component * shrink for component in stepped]
            renewed.append(projected)
            divergences.append(backward(projected[0], 0) + backward(projected[1], 1) + backward(projected[2], 2))
        dual_field = renewed
        fidelity = (volume[None] - centers[:, None, None, None]) ** 2
        updated = project_simplex(labelling + tau_step * (jnp.stack(divergences) - fidelity))
        smoothed = 2.0 * updated - labelling
        labelling = updated
        sizes_all = lax.optimization_barrier(jnp.sum(labelling, axis=(1, 2, 3)))
        weighted = lax.optimization_barrier(jnp.sum(labelling * volume[None], axis=(1, 2, 3)))
        centers = (weighted + prior_weight * base_levels) / (sizes_all + prior_weight)
    return (labelling, centers)
```

```python
import functools

import jax
import jax.numpy as jnp
from jax import lax
from jax.experimental import pallas as pl
from jax.experimental.pallas import tpu as pltpu
from jax.sharding import PartitionSpec as P

TAU = 0.25
SIGMA = 0.25
LAMBDA = 0.5
PRIOR = 1.0
HALO = 2
ROWS = 8
LANES = 128
MESH = pl.DeviceIdType.MESH


def project_simplex(v):
    a, b, c, d = v
    hi1, lo1 = jnp.maximum(a, b), jnp.minimum(a, b)
    hi2, lo2 = jnp.maximum(c, d), jnp.minimum(c, d)
    s1, s2 = a + b, c + d
    top1 = jnp.maximum(hi1, hi2)
    top2 = jnp.maximum(hi1 + hi2, jnp.maximum(s1, s2))
    top3 = jnp.maximum(s1 + hi2, s2 + hi1)
    top4 = s1 + s2
    t = jnp.maximum(
        jnp.maximum(top1 - 1.0, top2 * 0.5 - 0.5),
        jnp.maximum(top3 * (1.0 / 3.0) - (1.0 / 3.0), top4 * 0.25 - 0.25),
    )
    return [jnp.maximum(x - t, 0.0) for x in v]


def kernel(cfg, levels_ref, vol_ref, lab_ref, cen_ref, vin, buf, rows, volt, s1_ref, l1_ref, p_ref, l2_ref,
           stage, sum_src, sum_plane, sum_line, vin_sem, own_sem, x_send, x_recv, h_send, h_recv,
           z_send, z_recv, a_send, a_recv, out_sem):
    nx, ny, nz, G, X, Z, T = cfg
    how_many = 4
    lx, ly, lz = T * G, ny // G, LANES
    ye = ly + 2 * HALO
    xe = lx + 2 * HALO
    J = volt.shape[0]
    win = buf.shape[1] - 16
    gx, gy, gz = lax.axis_index("gx"), lax.axis_index("gy"), lax.axis_index("gz")
    tiles = lz // ROWS + 2

    load = pltpu.make_async_copy(vol_ref, vin, vin_sem)
    load.start()

    plane = X * G
    me_plane = gx * G + gy
    plane_peers = []
    for d in range(1, plane):
        q = lax.rem(me_plane + d, plane)
        plane_peers.append({"gx": q // G, "gy": lax.rem(q, G), "gz": gz})
    line_peers = [{"gx": gx, "gy": gy, "gz": lax.rem(gz + d, Z)} for d in range(1, Z)]
    barrier = pltpu.get_barrier_semaphore()
    for peer in plane_peers + line_peers:
        pl.semaphore_signal(barrier, inc=1, device_id=peer, device_id_type=MESH)
    pl.semaphore_wait(barrier, len(plane_peers) + len(line_peers))
    load.wait()

    def window(g):
        start = jnp.clip(g * ly - 8, 0, ny - win)
        return pl.multiple_of(start, 8), pl.multiple_of(start - (g * ly - 16), 8)

    sends = []
    for d in range(1, G):
        g = lax.rem(gy + d, G)
        src, dst = window(g)
        c = pltpu.make_async_remote_copy(
            vin.at[:, pl.ds(src, win), :], buf.at[pl.ds(HALO + gy * T, T), pl.ds(dst, win), :],
            x_send.at[d], x_recv.at[gy], device_id={"gx": gx, "gy": g, "gz": gz}, device_id_type=MESH)
        c.start()
        sends.append(c)

    def halo(up, g):
        src, dst = window(g)
        return pltpu.make_async_remote_copy(
            vin.at[pl.ds(T - HALO if up else 0, HALO), pl.ds(src, win), :],
            buf.at[pl.ds(0 if up else HALO + lx, HALO), pl.ds(dst, win), :],
            h_send.at[int(up), g], h_recv.at[int(up)],
            device_id={"gx": gx + 1 if up else gx - 1, "gy": g, "gz": gz}, device_id_type=MESH)

    send_up = (gy == G - 1) & (gx < X - 1)
    send_down = (gy == 0) & (gx > 0)

    @pl.when(send_up)
    def _():
        for g in range(G):
            halo(True, g).start()

    @pl.when(send_down)
    def _():
        for g in range(G):
            halo(False, g).start()

    src, dst = window(gy)
    own = pltpu.make_async_copy(
        vin.at[:, pl.ds(src, win), :], buf.at[pl.ds(HALO + gy * T, T), pl.ds(dst, win), :], own_sem)
    own.start()

    base = [levels_ref[l].astype(jnp.float32) * (1.0 / 255.0) for l in range(how_many)]
    row = lax.broadcasted_iota(jnp.int32, (ROWS, LANES), 0)
    lane = lax.broadcasted_iota(jnp.int32, (ROWS, LANES), 1)
    part, yloc = lane // ye, lane % ye
    x0, y0, z0 = gx * lx - HALO, gy * ly - HALO, gz * lz
    yg = y0 + yloc
    step = TAU * SIGMA
    my = jnp.where((yg >= 0) & (yg < ny - 1), step, 0.0)
    mx, inside, mine = [], [], []
    for j in range(J):
        xloc = part * J + j
        xg = x0 + xloc
        mx.append(jnp.where((xg >= 0) & (xg < nx - 1), step, 0.0))
        inside.append((xg >= 0) & (xg < nx) & (yg >= 0) & (yg < ny) & (xloc < xe))
        mine.append(jnp.where((xloc >= HALO) & (xloc < HALO + lx) & (yloc >= HALO) & (yloc < HALO + ly), 1.0, 0.0))

    def mz(i):
        zg = z0 + (i - 1) * ROWS + row
        return jnp.where((zg >= 0) & (zg < nz - 1), step, 0.0)

    own.wait()
    for d in range(1, G):
        g = lax.rem(gy + d, G)
        pltpu.make_async_remote_copy(
            vin.at[:, pl.ds(src, win), :], buf.at[pl.ds(HALO + g * T, T), pl.ds(dst, win), :],
            x_send.at[d], x_recv.at[g], device_id={"gx": gx, "gy": g, "gz": gz}, device_id_type=MESH).wait_recv()

    def halo_in(up):
        return pltpu.make_async_remote_copy(
            vin.at[pl.ds(0, HALO), pl.ds(src, win), :],
            buf.at[pl.ds(0 if up else HALO + lx, HALO), pl.ds(dst, win), :],
            h_send.at[int(up), 0], h_recv.at[int(up)],
            device_id={"gx": gx, "gy": lax.rem(gy + 1, G), "gz": gz}, device_id_type=MESH)

    @pl.when(gx > 0)
    def _():
        halo_in(True).wait_recv()

    @pl.when(gx < X - 1)
    def _():
        halo_in(False).wait_recv()

    for j in range(J):
        rows[j] = jnp.zeros((LANES, LANES), jnp.float32)
        for i in range(-(-(xe - j) // J)):
            rows[j, i * ye:(i + 1) * ye, :] = buf[i * J + j, 16 - HALO:16 - HALO + ye, :]
    for j in range(J):
        t = rows[j].T
        keep = jnp.broadcast_to(inside[j][:1], (LANES, LANES))
        volt[j, ROWS:ROWS + lz, :] = jnp.where(keep, t, 0.0)

    def z_copy(up):
        return pltpu.make_async_remote_copy(
            volt.at[:, pl.ds(lz if up else ROWS, ROWS), :],
            volt.at[:, pl.ds(0 if up else ROWS + lz, ROWS), :],
            z_send.at[int(up)], z_recv.at[int(up)],
            device_id={"gx": gx, "gy": gy, "gz": gz + 1 if up else gz - 1}, device_id_type=MESH)

    zero = jnp.zeros((J, ROWS, LANES), jnp.float32)

    @pl.when(gz < Z - 1)
    def _():
        z_copy(True).start()

    @pl.when(gz > 0)
    def _():
        z_copy(False).start()

    @pl.when(gz == 0)
    def _():
        volt[:, 0:ROWS, :] = zero

    @pl.when(gz == Z - 1)
    def _():
        volt[:, ROWS + lz:, :] = zero

    @pl.when(gz > 0)
    def _():
        z_copy(True).wait_recv()

    @pl.when(gz < Z - 1)
    def _():
        z_copy(False).wait_recv()

    def at(ref, l, j, i):
        return ref[l, j, pl.ds(pl.multiple_of(i * ROWS, ROWS), ROWS), :]

    def vtile(j, i):
        return volt[j, pl.ds(pl.multiple_of(i * ROWS, ROWS), ROWS), :]

    base_a = [2.0 * TAU * b for b in base]
    base_b = [TAU * b * b for b in base]

    def pull(v):
        return [base_a[l] * v - base_b[l] for l in range(how_many)]

    def start_labels(i):
        return [project_simplex(pull(vtile(j, i))) for j in range(J)]

    def dual_step(s, sn, before, mzi):
        sz = [pltpu.roll(jnp.where(row == 0, sn[j], s[j]), ROWS - 1, 0) for j in range(J)]
        sy = [pltpu.roll(s[j], LANES - 1, 1) for j in range(J)]
        sx = s[1:] + [pltpu.roll(s[0], LANES - ye, 1)]
        px, py, pz = [], [], []
        for j in range(J):
            ax, ay, az = mx[j] * (sx[j] - s[j]), my * (sy[j] - s[j]), mzi * (sz[j] - s[j])
            if before is not None:
                ax, ay, az = ax + before[0][j], ay + before[1][j], az + before[2][j]
            shrink = jnp.minimum(1.0, (TAU * LAMBDA) * lax.rsqrt(ax * ax + ay * ay + az * az))
            px.append(ax * shrink)
            py.append(ay * shrink)
            pz.append(az * shrink)
        return px, py, pz

    def divergence(px, py, pz, pz_before):
        bx = [pltpu.roll(px[J - 1], ye, 1)] + px[:-1]
        out = []
        for j in range(J):
            by = pltpu.roll(py[j], 1, 1)
            bz = pltpu.roll(jnp.where(row == ROWS - 1, pz_before[j], pz[j]), 1, 0)
            out.append(((px[j] - bx[j]) + (py[j] - by)) + (pz[j] - bz))
        return out

    nothing = jnp.zeros((ROWS, LANES), jnp.float32)

    def first(i, carry):
        lab, prev, acc = carry
        ahead = start_labels(jnp.minimum(i + 1, tiles - 1))
        mzi = mz(i)
        here = pl.ds(pl.multiple_of(i * ROWS, ROWS), ROWS)
        own_rows = jnp.where((i > 0) & (i < tiles - 1), 1.0, 0.0)
        u = [[] for j in range(J)]
        new_prev = []
        v = [vtile(j, i) for j in range(J)]
        w = [pull(v[j]) for j in range(J)]
        for l in range(how_many):
            s = [lab[j][l] for j in range(J)]
            px, py, pz = dual_step(s, [ahead[j][l] for j in range(J)], None, mzi)
            div = divergence(px, py, pz, prev[l])
            for j in range(J):
                p_ref[0, l, j, here, :] = px[j]
                p_ref[1, l, j, here, :] = py[j]
                p_ref[2, l, j, here, :] = pz[j]
                u[j].append(s[j] + (div[j] + w[j][l]))
            new_prev.append(pz)
        acc = list(acc)
        for j in range(J):
            new = project_simplex(u[j])
            m = mine[j] * own_rows
            vm = v[j] * m
            for l in range(how_many):
                l1_ref[l, j, here, :] = new[l]
                s1_ref[l, j, here, :] = 2.0 * new[l] - lab[j][l]
                acc[l] = acc[l] + new[l] * m
                acc[how_many + l] = acc[how_many + l] + new[l] * vm
        return ahead, new_prev, acc

    no_prev = [[nothing] * J for l in range(how_many)]
    _, _, acc = lax.fori_loop(0, tiles, first, (start_labels(0), no_prev, [nothing] * (2 * how_many)))

    def reduce_start(k, acc):
        sum_src[k, 0] = jnp.concatenate([jnp.sum(a, axis=0, keepdims=True) for a in acc], axis=0)
        sum_plane[k, me_plane] = sum_src[k, 0]
        out = []
        for d, peer in enumerate(plane_peers, 1):
            c = pltpu.make_async_remote_copy(
                sum_src.at[k, 0], sum_plane.at[k, me_plane], a_send.at[k, d], a_recv.at[k, me_plane],
                device_id=peer, device_id_type=MESH)
            c.start()
            out.append(c)
        return out

    def reduce_finish(k):
        out = []
        for d, peer in enumerate(plane_peers, 1):
            q = lax.rem(me_plane + d, plane)
            pltpu.make_async_remote_copy(
                sum_src.at[k, 0], sum_plane.at[k, q], a_send.at[k, d], a_recv.at[k, q],
                device_id=peer, device_id_type=MESH).wait_recv()
        total = sum_plane[k, 0]
        for q in range(1, plane):
            total = total + sum_plane[k, q]
        sum_src[k, 1] = total
        sum_line[k, gz] = total
        for d, peer in enumerate(line_peers, 1):
            c = pltpu.make_async_remote_copy(
                sum_src.at[k, 1], sum_line.at[k, gz], a_send.at[k, plane + d], a_recv.at[k, plane + gz],
                device_id=peer, device_id_type=MESH)
            c.start()
            out.append(c)
        for d, peer in enumerate(line_peers, 1):
            q = lax.rem(gz + d, Z)
            pltpu.make_async_remote_copy(
                sum_src.at[k, 1], sum_line.at[k, q], a_send.at[k, plane + d], a_recv.at[k, plane + q],
                device_id=peer, device_id_type=MESH).wait_recv()
        total = sum_line[k, 0]
        for q in range(1, Z):
            total = total + sum_line[k, q]
        total = jnp.broadcast_to(jnp.sum(total, axis=1, keepdims=True), (ROWS, LANES))
        centers = []
        for l in range(how_many):
            size, weighted = total[l:l + 1], total[how_many + l:how_many + l + 1]
            centers.append((weighted + PRIOR * base[l]) / (size + PRIOR))
        return centers, out

    sends += reduce_start(0, acc)

    def second(i, prev):
        mzi = mz(i)
        here = pl.ds(pl.multiple_of(i * ROWS, ROWS), ROWS)
        new_prev = []
        for l in range(how_many):
            s = [at(s1_ref, l, j, i) for j in range(J)]
            sn = [at(s1_ref, l, j, i + 1) for j in range(J)]
            before = [[p_ref[k, l, j, here, :] for j in range(J)] for k in range(3)]
            px, py, pz = dual_step(s, sn, before, mzi)
            div = divergence(px, py, pz, prev[l])
            for j in range(J):
                l1_ref[l, j, here, :] = l1_ref[l, j, here, :] + div[j]
            new_prev.append(pz)
        return new_prev

    lax.fori_loop(0, tiles - 1, second, no_prev)

    centers, more = reduce_finish(0)
    sends += more
    cen_a = [jnp.broadcast_to(2.0 * TAU * c, (ROWS, LANES)) for c in centers]
    cen_b = [jnp.broadcast_to(TAU * c * c, (ROWS, LANES)) for c in centers]

    def third(i, acc):
        acc = list(acc)
        there = pl.ds(pl.multiple_of((i - 1) * ROWS, ROWS), ROWS)
        for j in range(J):
            v = vtile(j, i)
            new = project_simplex([at(l1_ref, l, j, i) + (cen_a[l] * v - cen_b[l]) for l in range(how_many)])
            vm = v * mine[j]
            for l in range(how_many):
                l2_ref[l, j, there, :] = new[l]
                acc[l] = acc[l] + new[l] * mine[j]
                acc[how_many + l] = acc[how_many + l] + new[l] * vm
        return acc

    acc = lax.fori_loop(1, tiles - 1, third, [nothing] * (2 * how_many))
    sends += reduce_start(1, acc)

    outs = []
    for l in range(how_many):
        for j in range(J):
            rows[j] = l2_ref[l, j].T
            for i in range(-(-(xe - j) // J)):
                x = i * J + j - HALO
                if 0 <= x < lx:
                    stage[l, x] = rows[j, i * ye + HALO:i * ye + HALO + ly, :]
        c = pltpu.make_async_copy(stage.at[l], lab_ref.at[l], out_sem.at[l])
        c.start()
        outs.append(c)

    centers, more = reduce_finish(1)
    sends += more
    for l in range(how_many):
        cen_ref[l] = centers[l][0, 0]
    for c in outs:
        c.wait()
    for c in sends:
        c.wait_send()

    @pl.when(send_up)
    def _():
        for g in range(G):
            halo(True, g).wait_send()

    @pl.when(send_down)
    def _():
        for g in range(G):
            halo(False, g).wait_send()

    @pl.when(gz < Z - 1)
    def _():
        z_copy(True).wait_send()

    @pl.when(gz > 0)
    def _():
        z_copy(False).wait_send()


def solution(mesh):
    X, G, Z = mesh.shape["gx"], mesh.shape["gy"], mesh.shape["gz"]

    def local(volume, levels):
        T, ny, lz = volume.shape
        nx, nz = T * X * G, lz * Z
        lx, ly = T * G, ny // G
        ye, xe = ly + 2 * HALO, lx + 2 * HALO
        J = -(-xe // (LANES // ye))
        win = min(ny, ly + 16)
        n = levels.shape[0]
        f32 = jnp.float32
        dma = pltpu.SemaphoreType.DMA
        zrows = lz + 2 * ROWS
        return pl.pallas_call(
            functools.partial(kernel, (nx, ny, nz, G, X, Z, T)),
            out_shape=(jax.ShapeDtypeStruct((n, lx, ly, lz), f32), jax.ShapeDtypeStruct((n,), f32)),
            in_specs=[pl.BlockSpec(memory_space=pltpu.SMEM), pl.BlockSpec(memory_space=pl.ANY)],
            out_specs=(pl.BlockSpec(memory_space=pl.ANY), pl.BlockSpec(memory_space=pltpu.SMEM)),
            scratch_shapes=[
                pltpu.VMEM((T, ny, lz), f32),
                pltpu.VMEM((xe, win + 16, lz), f32),
                pltpu.VMEM((J, LANES, LANES), f32),
                pltpu.VMEM((J, zrows, LANES), f32),
                pltpu.VMEM((n, J, zrows, LANES), f32),
                pltpu.VMEM((n, J, zrows, LANES), f32),
                pltpu.VMEM((3, n, J, zrows, LANES), f32),
                pltpu.VMEM((n, J, lz, LANES), f32),
                pltpu.VMEM((n, lx, ly, lz), f32),
                pltpu.VMEM((2, 2, ROWS, LANES), f32),
                pltpu.VMEM((2, X * G, ROWS, LANES), f32),
                pltpu.VMEM((2, Z, ROWS, LANES), f32),
                dma, dma, dma((G,)), dma((G,)), dma((2, G)), dma((2,)), dma((2,)), dma((2,)),
                dma((2, X * G + Z)), dma((2, X * G + Z)), dma((n,)),
            ],
            compiler_params=pltpu.CompilerParams(collective_id=0, has_side_effects=True),
        )(levels, volume)

    return jax.shard_map(
        local,
        mesh=mesh,
        in_specs=(P(("gx", "gy"), None, "gz"), P()),
        out_specs=(P(None, "gx", "gy", "gz"), P()),
        check_vma=False,
    )
```

```python
import functools

import jax
import jax.numpy as jnp
from jax import lax
from jax.experimental import pallas as pl
from jax.experimental.pallas import tpu as pltpu
from jax.sharding import PartitionSpec as P

TAU = 0.25
SIGMA = 0.25
LAMBDA = 0.5
PRIOR = 1.0
HALO = 2
ROWS = 8
LANES = 128
MESH = pl.DeviceIdType.MESH


def project_simplex(v):
    a, b, c, d = v
    hi1, lo1 = jnp.maximum(a, b), jnp.minimum(a, b)
    hi2, lo2 = jnp.maximum(c, d), jnp.minimum(c, d)
    s1, s2 = a + b, c + d
    top1 = jnp.maximum(hi1, hi2)
    top2 = jnp.maximum(hi1 + hi2, jnp.maximum(s1, s2))
    top3 = jnp.maximum(s1 + hi2, s2 + hi1)
    top4 = s1 + s2
    t = jnp.maximum(
        jnp.maximum(top1 - 1.0, top2 * 0.5 - 0.5),
        jnp.maximum(top3 * (1.0 / 3.0) - (1.0 / 3.0), top4 * 0.25 - 0.25),
    )
    return [jnp.maximum(x - t, 0.0) for x in v]


def kernel(cfg, levels_ref, vol_ref, lab_ref, cen_ref, vin, buf, rows, volt, s1_ref, l1_ref, p_ref, l2_ref,
           stage, sum_src, sum_all, vin_sem, own_sem, x_send, x_recv, h_send, h_recv,
           z_send, z_recv, a_send, a_recv, out_sem, far):
    nx, ny, nz, G, X, Z, T = cfg
    how_many = 4
    lx, ly, lz = T * G, ny // G, LANES
    ye = ly + 2 * HALO
    xe = lx + 2 * HALO
    J = volt.shape[0]
    win = buf.shape[1] - 16
    gx, gy, gz = lax.axis_index("gx"), lax.axis_index("gy"), lax.axis_index("gz")
    tiles = lz // ROWS + 2

    load = pltpu.make_async_copy(vol_ref, vin, vin_sem)
    load.start()

    plane = X * G
    me_plane = gx * G + gy
    plane_peers = []
    for d in range(1, plane):
        q = lax.rem(me_plane + d, plane)
        plane_peers.append({"gx": q // G, "gy": lax.rem(q, G), "gz": gz})
    barrier = pltpu.get_barrier_semaphore()
    for peer in plane_peers:
        pl.semaphore_signal(barrier, inc=1, device_id=peer, device_id_type=MESH)
    above = {"gx": gx, "gy": gy, "gz": gz + 1}
    below = {"gx": gx, "gy": gy, "gz": gz - 1}
    has_above, has_below = gz < Z - 1, gz > 0

    @pl.when(has_above)
    def _():
        pl.semaphore_signal(barrier, inc=1, device_id=above, device_id_type=MESH)

    @pl.when(has_below)
    def _():
        pl.semaphore_signal(barrier, inc=1, device_id=below, device_id_type=MESH)

    pl.semaphore_wait(barrier, plane - 1 + has_above.astype(jnp.int32) + has_below.astype(jnp.int32))
    load.wait()

    def window(g):
        start = jnp.clip(g * ly - 8, 0, ny - win)
        return pl.multiple_of(start, 8), pl.multiple_of(start - (g * ly - 16), 8)

    sends = []
    for d in range(1, G):
        g = lax.rem(gy + d, G)
        src, dst = window(g)
        c = pltpu.make_async_remote_copy(
            vin.at[:, pl.ds(src, win), :], buf.at[pl.ds(HALO + gy * T, T), pl.ds(dst, win), :],
            x_send.at[d], x_recv.at[gy], device_id={"gx": gx, "gy": g, "gz": gz}, device_id_type=MESH)
        c.start()
        sends.append(c)

    def halo(up, g):
        src, dst = window(g)
        return pltpu.make_async_remote_copy(
            vin.at[pl.ds(T - HALO if up else 0, HALO), pl.ds(src, win), :],
            buf.at[pl.ds(0 if up else HALO + lx, HALO), pl.ds(dst, win), :],
            h_send.at[int(up), g], h_recv.at[int(up)],
            device_id={"gx": gx + 1 if up else gx - 1, "gy": g, "gz": gz}, device_id_type=MESH)

    send_up = (gy == G - 1) & (gx < X - 1)
    send_down = (gy == 0) & (gx > 0)

    @pl.when(send_up)
    def _():
        for g in range(G):
            halo(True, g).start()

    @pl.when(send_down)
    def _():
        for g in range(G):
            halo(False, g).start()

    @pl.when(jnp.logical_not(has_below) & has_above)
    def _():
        pl.semaphore_signal(far.at[1], inc=1, device_id=above, device_id_type=MESH)

    @pl.when(has_above)
    def _():
        pl.semaphore_wait(far.at[0], 1)

    @pl.when(has_below)
    def _():
        pl.semaphore_signal(far.at[0], inc=1, device_id=below, device_id_type=MESH)
        pl.semaphore_wait(far.at[1], 1)

    @pl.when(has_below & has_above)
    def _():
        pl.semaphore_signal(far.at[1], inc=1, device_id=above, device_id_type=MESH)

    src, dst = window(gy)
    own = pltpu.make_async_copy(
        vin.at[:, pl.ds(src, win), :], buf.at[pl.ds(HALO + gy * T, T), pl.ds(dst, win), :], own_sem)
    own.start()

    base = [levels_ref[l].astype(jnp.float32) * (1.0 / 255.0) for l in range(how_many)]
    row = lax.broadcasted_iota(jnp.int32, (ROWS, LANES), 0)
    lane = lax.broadcasted_iota(jnp.int32, (ROWS, LANES), 1)
    part, yloc = lane // ye, lane % ye
    x0, y0, z0 = gx * lx - HALO, gy * ly - HALO, gz * lz
    yg = y0 + yloc
    step = TAU * SIGMA
    my = jnp.where((yg >= 0) & (yg < ny - 1), step, 0.0)
    mx, inside, mine = [], [], []
    for j in range(J):
        xloc = part * J + j
        xg = x0 + xloc
        mx.append(jnp.where((xg >= 0) & (xg < nx - 1), step, 0.0))
        inside.append((xg >= 0) & (xg < nx) & (yg >= 0) & (yg < ny) & (xloc < xe))
        mine.append(jnp.where((xloc >= HALO) & (xloc < HALO + lx) & (yloc >= HALO) & (yloc < HALO + ly), 1.0, 0.0))

    def mz(i):
        zg = z0 + (i - 1) * ROWS + row
        return jnp.where((zg >= 0) & (zg < nz - 1), step, 0.0)

    own.wait()
    for d in range(1, G):
        g = lax.rem(gy + d, G)
        pltpu.make_async_remote_copy(
            vin.at[:, pl.ds(src, win), :], buf.at[pl.ds(HALO + g * T, T), pl.ds(dst, win), :],
            x_send.at[d], x_recv.at[g], device_id={"gx": gx, "gy": g, "gz": gz}, device_id_type=MESH).wait_recv()

    def halo_in(up):
        return pltpu.make_async_remote_copy(
            vin.at[pl.ds(0, HALO), pl.ds(src, win), :],
            buf.at[pl.ds(0 if up else HALO + lx, HALO), pl.ds(dst, win), :],
            h_send.at[int(up), 0], h_recv.at[int(up)],
            device_id={"gx": gx, "gy": lax.rem(gy + 1, G), "gz": gz}, device_id_type=MESH)

    @pl.when(gx > 0)
    def _():
        halo_in(True).wait_recv()

    @pl.when(gx < X - 1)
    def _():
        halo_in(False).wait_recv()

    for j in range(J):
        rows[j] = jnp.zeros((LANES, LANES), jnp.float32)
        for i in range(-(-(xe - j) // J)):
            rows[j, i * ye:(i + 1) * ye, :] = buf[i * J + j, 16 - HALO:16 - HALO + ye, :]
    for j in range(J):
        t = rows[j].T
        keep = jnp.broadcast_to(inside[j][:1], (LANES, LANES))
        volt[j, ROWS:ROWS + lz, :] = jnp.where(keep, t, 0.0)

    def z_copy(up):
        return pltpu.make_async_remote_copy(
            volt.at[:, pl.ds(lz if up else ROWS, ROWS), :],
            volt.at[:, pl.ds(0 if up else ROWS + lz, ROWS), :],
            z_send.at[int(up)], z_recv.at[int(up)],
            device_id={"gx": gx, "gy": gy, "gz": gz + 1 if up else gz - 1}, device_id_type=MESH)

    zero = jnp.zeros((J, ROWS, LANES), jnp.float32)

    @pl.when(gz < Z - 1)
    def _():
        z_copy(True).start()

    @pl.when(gz > 0)
    def _():
        z_copy(False).start()

    @pl.when(gz == 0)
    def _():
        volt[:, 0:ROWS, :] = zero

    @pl.when(gz == Z - 1)
    def _():
        volt[:, ROWS + lz:, :] = zero

    def at(ref, l, j, i):
        return ref[l, j, pl.ds(pl.multiple_of(i * ROWS, ROWS), ROWS), :]

    def vtile(j, i):
        return volt[j, pl.ds(pl.multiple_of(i * ROWS, ROWS), ROWS), :]

    base_a = [2.0 * TAU * b for b in base]
    base_b = [TAU * b * b for b in base]

    def pull(v):
        return [base_a[l] * v - base_b[l] for l in range(how_many)]

    def start_labels(i):
        return [project_simplex(pull(vtile(j, i))) for j in range(J)]

    def dual_step(s, sn, before, mzi):
        sz = [pltpu.roll(jnp.where(row == 0, sn[j], s[j]), ROWS - 1, 0) for j in range(J)]
        sy = [pltpu.roll(s[j], LANES - 1, 1) for j in range(J)]
        sx = s[1:] + [pltpu.roll(s[0], LANES - ye, 1)]
        px, py, pz = [], [], []
        for j in range(J):
            ax, ay, az = mx[j] * (sx[j] - s[j]), my * (sy[j] - s[j]), mzi * (sz[j] - s[j])
            if before is not None:
                ax, ay, az = ax + before[0][j], ay + before[1][j], az + before[2][j]
            shrink = jnp.minimum(1.0, (TAU * LAMBDA) * lax.rsqrt(ax * ax + ay * ay + az * az))
            px.append(ax * shrink)
            py.append(ay * shrink)
            pz.append(az * shrink)
        return px, py, pz

    def divergence(px, py, pz, pz_before):
        bx = [pltpu.roll(px[J - 1], ye, 1)] + px[:-1]
        out = []
        for j in range(J):
            by = pltpu.roll(py[j], 1, 1)
            bz = pltpu.roll(jnp.where(row == ROWS - 1, pz_before[j], pz[j]), 1, 0)
            out.append(((px[j] - bx[j]) + (py[j] - by)) + (pz[j] - bz))
        return out

    nothing = jnp.zeros((ROWS, LANES), jnp.float32)

    def first(i, carry):
        lab, prev, acc = carry
        ahead = start_labels(jnp.minimum(i + 1, tiles - 1))
        mzi = mz(i)
        here = pl.ds(pl.multiple_of(i * ROWS, ROWS), ROWS)
        own_rows = jnp.where((i > 0) & (i < tiles - 1), 1.0, 0.0)
        u = [[] for j in range(J)]
        new_prev = []
        v = [vtile(j, i) for j in range(J)]
        w = [pull(v[j]) for j in range(J)]
        for l in range(how_many):
            s = [lab[j][l] for j in range(J)]
            px, py, pz = dual_step(s, [ahead[j][l] for j in range(J)], None, mzi)
            div = divergence(px, py, pz, prev[l])
            for j in range(J):
                p_ref[0, l, j, here, :] = px[j]
                p_ref[1, l, j, here, :] = py[j]
                p_ref[2, l, j, here, :] = pz[j]
                u[j].append(s[j] + (div[j] + w[j][l]))
            new_prev.append(pz)
        acc = list(acc)
        for j in range(J):
            new = project_simplex(u[j])
            m = mine[j] * own_rows
            vm = v[j] * m
            for l in range(how_many):
                l1_ref[l, j, here, :] = new[l]
                s1_ref[l, j, here, :] = 2.0 * new[l] - lab[j][l]
                acc[l] = acc[l] + new[l] * m
                acc[how_many + l] = acc[how_many + l] + new[l] * vm
        return ahead, new_prev, acc

    no_prev = [[nothing] * J for l in range(how_many)]
    one, two = start_labels(1), start_labels(2)
    prev = [dual_step([one[j][l] for j in range(J)], [two[j][l] for j in range(J)], None, mz(1))[2]
            for l in range(how_many)]
    _, _, acc = carry = lax.fori_loop(2, tiles - 2, first, (two, prev, [nothing] * (2 * how_many)))

    @pl.when(gz > 0)
    def _():
        z_copy(True).wait_recv()

    @pl.when(gz < Z - 1)
    def _():
        z_copy(False).wait_recv()

    _, _, acc = lax.fori_loop(tiles - 2, tiles, first, (start_labels(tiles - 2), carry[1], acc))
    _, _, acc = lax.fori_loop(0, 2, first, (start_labels(0), no_prev, acc))

    N = X * G * Z
    me = me_plane * Z + gz
    xs = [lax.rem(gx + d, X) for d in range(X)]
    gs = [lax.rem(gy + d, G) for d in range(G)]
    zs = [lax.rem(gz + d, Z) for d in range(Z)]
    offsets = [(a, b, c) for a in range(X) for b in range(G) for c in range(Z)][:0:-1]

    def reduce_start(k, acc):
        t = jnp.concatenate([jnp.sum(a, axis=0, keepdims=True) for a in acc], axis=0)
        t = jnp.where(row == lane, jnp.sum(t, axis=1, keepdims=True), 0.0)
        t = jnp.sum(t, axis=0, keepdims=True)
        sum_src[k] = t
        sum_all[k, me] = t
        for a, b, c in offsets:
            pltpu.make_async_remote_copy(
                sum_src.at[k], sum_all.at[k, me], a_send.at[k], a_recv.at[k],
                device_id={"gx": xs[a], "gy": gs[b], "gz": zs[c]}, device_id_type=MESH).start()

    def every(k):
        part = sum_all.at[k, pl.ds(0, N - 1)]
        return pltpu.make_async_remote_copy(
            part, part, a_send.at[k], a_recv.at[k],
            device_id={"gx": xs[-1], "gy": gs[-1], "gz": zs[-1]}, device_id_type=MESH)

    def reduce_finish(k):
        every(k).wait_recv()
        terms = [sum_all[k, q] for q in range(N)]
        while len(terms) > 1:
            terms = [sum(terms[q:q + 2][1:], terms[q]) for q in range(0, len(terms), 2)]
        total = terms[0]
        start = jnp.zeros((1, LANES), jnp.float32)
        for l in range(how_many):
            start = jnp.where(lane[:1] == l, PRIOR * base[l], start)
        return (pltpu.roll(total, LANES - how_many, 1) + start) / (total + PRIOR)

    reduce_start(0, acc)

    def second(i, prev):
        mzi = mz(i)
        here = pl.ds(pl.multiple_of(i * ROWS, ROWS), ROWS)
        new_prev = []
        for l in range(how_many):
            s = [at(s1_ref, l, j, i) for j in range(J)]
            sn = [at(s1_ref, l, j, i + 1) for j in range(J)]
            before = [[p_ref[k, l, j, here, :] for j in range(J)] for k in range(3)]
            px, py, pz = dual_step(s, sn, before, mzi)
            div = divergence(px, py, pz, prev[l])
            for j in range(J):
                l1_ref[l, j, here, :] = l1_ref[l, j, here, :] + div[j]
            new_prev.append(pz)
        return new_prev

    lax.fori_loop(0, tiles - 1, second, no_prev)

    centers = reduce_finish(0)
    centers = [jnp.broadcast_to(centers[:, l:l + 1], (ROWS, LANES)) for l in range(how_many)]
    cen_a = [2.0 * TAU * c for c in centers]
    cen_b = [TAU * c * c for c in centers]

    def third(i, acc):
        acc = list(acc)
        there = pl.ds(pl.multiple_of((i - 1) * ROWS, ROWS), ROWS)
        for j in range(J):
            v = vtile(j, i)
            new = project_simplex([at(l1_ref, l, j, i) + (cen_a[l] * v - cen_b[l]) for l in range(how_many)])
            vm = v * mine[j]
            for l in range(how_many):
                l2_ref[l, j, there, :] = new[l]
                acc[l] = acc[l] + new[l] * mine[j]
                acc[how_many + l] = acc[how_many + l] + new[l] * vm
        return acc

    acc = lax.fori_loop(1, tiles - 1, third, [nothing] * (2 * how_many))
    reduce_start(1, acc)

    outs = []
    for l in range(how_many):
        for j in range(J):
            rows[j] = l2_ref[l, j].T
            for i in range(-(-(xe - j) // J)):
                x = i * J + j - HALO
                if 0 <= x < lx:
                    stage[l, x] = rows[j, i * ye + HALO:i * ye + HALO + ly, :]
        c = pltpu.make_async_copy(stage.at[l], lab_ref.at[l], out_sem.at[l])
        c.start()
        outs.append(c)

    centers = reduce_finish(1)
    for l in range(how_many):
        cen_ref[l] = centers[0, l]
    for c in outs:
        c.wait()
    for c in sends:
        c.wait_send()
    every(0).wait_send()
    every(1).wait_send()

    @pl.when(send_up)
    def _():
        for g in range(G):
            halo(True, g).wait_send()

    @pl.when(send_down)
    def _():
        for g in range(G):
            halo(False, g).wait_send()

    @pl.when(gz < Z - 1)
    def _():
        z_copy(True).wait_send()

    @pl.when(gz > 0)
    def _():
        z_copy(False).wait_send()


def solution(mesh):
    X, G, Z = mesh.shape["gx"], mesh.shape["gy"], mesh.shape["gz"]

    def local(volume, levels):
        T, ny, lz = volume.shape
        nx, nz = T * X * G, lz * Z
        lx, ly = T * G, ny // G
        ye, xe = ly + 2 * HALO, lx + 2 * HALO
        J = -(-xe // (LANES // ye))
        win = min(ny, ly + 16)
        n = levels.shape[0]
        f32 = jnp.float32
        dma = pltpu.SemaphoreType.DMA
        zrows = lz + 2 * ROWS
        return pl.pallas_call(
            functools.partial(kernel, (nx, ny, nz, G, X, Z, T)),
            out_shape=(jax.ShapeDtypeStruct((n, lx, ly, lz), f32), jax.ShapeDtypeStruct((n,), f32)),
            in_specs=[pl.BlockSpec(memory_space=pltpu.SMEM), pl.BlockSpec(memory_space=pl.ANY)],
            out_specs=(pl.BlockSpec(memory_space=pl.ANY), pl.BlockSpec(memory_space=pltpu.SMEM)),
            scratch_shapes=[
                pltpu.VMEM((T, ny, lz), f32),
                pltpu.VMEM((xe, win + 16, lz), f32),
                pltpu.VMEM((J, LANES, LANES), f32),
                pltpu.VMEM((J, zrows, LANES), f32),
                pltpu.VMEM((n, J, zrows, LANES), f32),
                pltpu.VMEM((n, J, zrows, LANES), f32),
                pltpu.VMEM((3, n, J, zrows, LANES), f32),
                pltpu.VMEM((n, J, lz, LANES), f32),
                pltpu.VMEM((n, lx, ly, lz), f32),
                pltpu.VMEM((2, 1, LANES), f32),
                pltpu.VMEM((2, X * G * Z, 1, LANES), f32),
                dma, dma, dma((G,)), dma((G,)), dma((2, G)), dma((2,)), dma((2,)), dma((2,)),
                dma((2,)), dma((2,)), dma((n,)), pltpu.SemaphoreType.REGULAR((2,)),
            ],
            compiler_params=pltpu.CompilerParams(collective_id=0, has_side_effects=True),
        )(levels, volume)

    return jax.shard_map(
        local,
        mesh=mesh,
        in_specs=(P(("gx", "gy"), None, "gz"), P()),
        out_specs=(P(None, "gx", "gy", "gz"), P()),
        check_vma=False,
    )
```

```python
import functools

import jax
import jax.numpy as jnp
from jax import lax
from jax.experimental import pallas as pl
from jax.experimental.pallas import tpu as pltpu
from jax.sharding import PartitionSpec as P

TAU = 0.25
SIGMA = 0.25
LAMBDA = 0.5
PRIOR = 1.0
HALO = 2
ROWS = 8
LANES = 128
MESH = pl.DeviceIdType.MESH


def project_simplex(v):
    a, b, c, d = v
    hi1, lo1 = jnp.maximum(a, b), jnp.minimum(a, b)
    hi2, lo2 = jnp.maximum(c, d), jnp.minimum(c, d)
    s1, s2 = a + b, c + d
    top1 = jnp.maximum(hi1, hi2)
    top2 = jnp.maximum(hi1 + hi2, jnp.maximum(s1, s2))
    top3 = jnp.maximum(s1 + hi2, s2 + hi1)
    top4 = s1 + s2
    t = jnp.maximum(
        jnp.maximum(top1 - 1.0, top2 * 0.5 - 0.5),
        jnp.maximum(top3 * (1.0 / 3.0) - (1.0 / 3.0), top4 * 0.25 - 0.25),
    )
    return [jnp.maximum(x - t, 0.0) for x in v]


def kernel(cfg, levels_hbm, vol_ref, lab_ref, cen_ref, vin, buf, rows, volt, s1_ref, l1_ref, p_ref, l2_ref,
           levels, sum_src, sum_all, vin_sem, own_sem, x_send, x_recv, h_send, h_recv,
           z_send, z_recv, a_send, a_recv, lev_sem, far):
    nx, ny, nz, G, X, Z, T = cfg
    how_many = 4
    lx, ly, lz = T * G, ny // G, LANES
    ye = ly + 2 * HALO
    xe = lx + 2 * HALO
    J = volt.shape[0]
    win = buf.shape[1] - 16
    gx, gy, gz = lax.axis_index("gx"), lax.axis_index("gy"), lax.axis_index("gz")
    tiles = lz // ROWS + 2

    load = pltpu.make_async_copy(vol_ref, vin, vin_sem)
    load.start()
    load_levels = pltpu.make_async_copy(levels_hbm, levels, lev_sem)
    load_levels.start()

    plane = X * G
    me_plane = gx * G + gy
    plane_peers = []
    for d in range(1, plane):
        q = lax.rem(me_plane + d, plane)
        plane_peers.append({"gx": q // G, "gy": lax.rem(q, G), "gz": gz})
    barrier = pltpu.get_barrier_semaphore()
    for peer in plane_peers:
        pl.semaphore_signal(barrier, inc=1, device_id=peer, device_id_type=MESH)
    above = {"gx": gx, "gy": gy, "gz": gz + 1}
    below = {"gx": gx, "gy": gy, "gz": gz - 1}
    has_above, has_below = gz < Z - 1, gz > 0

    @pl.when(has_above)
    def _():
        pl.semaphore_signal(barrier, inc=1, device_id=above, device_id_type=MESH)

    @pl.when(has_below)
    def _():
        pl.semaphore_signal(barrier, inc=1, device_id=below, device_id_type=MESH)

    pl.semaphore_wait(barrier, plane - 1 + has_above.astype(jnp.int32) + has_below.astype(jnp.int32))
    load.wait()

    def window(g):
        start = jnp.clip(g * ly - 8, 0, ny - win)
        return pl.multiple_of(start, 8), pl.multiple_of(start - (g * ly - 16), 8)

    sends = []
    for d in range(1, G):
        g = lax.rem(gy + d, G)
        src, dst = window(g)
        c = pltpu.make_async_remote_copy(
            vin.at[:, pl.ds(src, win), :], buf.at[pl.ds(HALO + gy * T, T), pl.ds(dst, win), :],
            x_send.at[d], x_recv.at[gy], device_id={"gx": gx, "gy": g, "gz": gz}, device_id_type=MESH)
        c.start()
        sends.append(c)

    def halo(up, g):
        src, dst = window(g)
        return pltpu.make_async_remote_copy(
            vin.at[pl.ds(T - HALO if up else 0, HALO), pl.ds(src, win), :],
            buf.at[pl.ds(0 if up else HALO + lx, HALO), pl.ds(dst, win), :],
            h_send.at[int(up), g], h_recv.at[int(up)],
            device_id={"gx": gx + 1 if up else gx - 1, "gy": g, "gz": gz}, device_id_type=MESH)

    send_up = (gy == G - 1) & (gx < X - 1)
    send_down = (gy == 0) & (gx > 0)

    @pl.when(send_up)
    def _():
        for g in range(G):
            halo(True, g).start()

    @pl.when(send_down)
    def _():
        for g in range(G):
            halo(False, g).start()

    @pl.when(jnp.logical_not(has_below) & has_above)
    def _():
        pl.semaphore_signal(far.at[1], inc=1, device_id=above, device_id_type=MESH)

    @pl.when(has_above)
    def _():
        pl.semaphore_wait(far.at[0], 1)

    @pl.when(has_below)
    def _():
        pl.semaphore_signal(far.at[0], inc=1, device_id=below, device_id_type=MESH)
        pl.semaphore_wait(far.at[1], 1)

    @pl.when(has_below & has_above)
    def _():
        pl.semaphore_signal(far.at[1], inc=1, device_id=above, device_id_type=MESH)

    src, dst = window(gy)
    own = pltpu.make_async_copy(
        vin.at[:, pl.ds(src, win), :], buf.at[pl.ds(HALO + gy * T, T), pl.ds(dst, win), :], own_sem)
    own.start()

    load_levels.wait()
    base = [levels[l].astype(jnp.float32) * (1.0 / 255.0) for l in range(how_many)]
    row = lax.broadcasted_iota(jnp.int32, (ROWS, LANES), 0)
    lane = lax.broadcasted_iota(jnp.int32, (ROWS, LANES), 1)
    part, yloc = lane // ye, lane % ye
    x0, y0, z0 = gx * lx - HALO, gy * ly - HALO, gz * lz
    yg = y0 + yloc
    step = TAU * SIGMA
    my = jnp.where((yg >= 0) & (yg < ny - 1), step, 0.0)
    mx, inside, mine = [], [], []
    for j in range(J):
        xloc = part * J + j
        xg = x0 + xloc
        mx.append(jnp.where((xg >= 0) & (xg < nx - 1), step, 0.0))
        inside.append((xg >= 0) & (xg < nx) & (yg >= 0) & (yg < ny) & (xloc < xe))
        mine.append(jnp.where((xloc >= HALO) & (xloc < HALO + lx) & (yloc >= HALO) & (yloc < HALO + ly), 1.0, 0.0))

    def mz(i):
        zg = z0 + (i - 1) * ROWS + row
        return jnp.where((zg >= 0) & (zg < nz - 1), step, 0.0)

    own.wait()
    for d in range(1, G):
        g = lax.rem(gy + d, G)
        pltpu.make_async_remote_copy(
            vin.at[:, pl.ds(src, win), :], buf.at[pl.ds(HALO + g * T, T), pl.ds(dst, win), :],
            x_send.at[d], x_recv.at[g], device_id={"gx": gx, "gy": g, "gz": gz}, device_id_type=MESH).wait_recv()

    def halo_in(up):
        return pltpu.make_async_remote_copy(
            vin.at[pl.ds(0, HALO), pl.ds(src, win), :],
            buf.at[pl.ds(0 if up else HALO + lx, HALO), pl.ds(dst, win), :],
            h_send.at[int(up), 0], h_recv.at[int(up)],
            device_id={"gx": gx, "gy": lax.rem(gy + 1, G), "gz": gz}, device_id_type=MESH)

    @pl.when(gx > 0)
    def _():
        halo_in(True).wait_recv()

    @pl.when(gx < X - 1)
    def _():
        halo_in(False).wait_recv()

    for j in range(J):
        rows[j] = jnp.zeros((LANES, LANES), jnp.float32)
        for i in range(-(-(xe - j) // J)):
            rows[j, i * ye:(i + 1) * ye, :] = buf[i * J + j, 16 - HALO:16 - HALO + ye, :]
    for j in range(J):
        t = rows[j].T
        keep = jnp.broadcast_to(inside[j][:1], (LANES, LANES))
        volt[j, ROWS:ROWS + lz, :] = jnp.where(keep, t, 0.0)

    def z_copy(up):
        return pltpu.make_async_remote_copy(
            volt.at[:, pl.ds(lz if up else ROWS, ROWS), :],
            volt.at[:, pl.ds(0 if up else ROWS + lz, ROWS), :],
            z_send.at[int(up)], z_recv.at[int(up)],
            device_id={"gx": gx, "gy": gy, "gz": gz + 1 if up else gz - 1}, device_id_type=MESH)

    zero = jnp.zeros((J, ROWS, LANES), jnp.float32)

    @pl.when(gz < Z - 1)
    def _():
        z_copy(True).start()

    @pl.when(gz > 0)
    def _():
        z_copy(False).start()

    @pl.when(gz == 0)
    def _():
        volt[:, 0:ROWS, :] = zero

    @pl.when(gz == Z - 1)
    def _():
        volt[:, ROWS + lz:, :] = zero

    def at(ref, l, j, i):
        return ref[l, j, pl.ds(pl.multiple_of(i * ROWS, ROWS), ROWS), :]

    def vtile(j, i):
        return volt[j, pl.ds(pl.multiple_of(i * ROWS, ROWS), ROWS), :]

    base_a = [2.0 * TAU * b for b in base]
    base_b = [TAU * b * b for b in base]

    def pull(v):
        return [base_a[l] * v - base_b[l] for l in range(how_many)]

    def start_labels(i):
        return [project_simplex(pull(vtile(j, i))) for j in range(J)]

    def dual_step(s, sn, before, mzi):
        sz = [pltpu.roll(jnp.where(row == 0, sn[j], s[j]), ROWS - 1, 0) for j in range(J)]
        sy = [pltpu.roll(s[j], LANES - 1, 1) for j in range(J)]
        sx = s[1:] + [pltpu.roll(s[0], LANES - ye, 1)]
        px, py, pz = [], [], []
        for j in range(J):
            ax, ay, az = mx[j] * (sx[j] - s[j]), my * (sy[j] - s[j]), mzi * (sz[j] - s[j])
            if before is not None:
                ax, ay, az = ax + before[0][j], ay + before[1][j], az + before[2][j]
            shrink = jnp.minimum(1.0, (TAU * LAMBDA) * lax.rsqrt(ax * ax + ay * ay + az * az))
            px.append(ax * shrink)
            py.append(ay * shrink)
            pz.append(az * shrink)
        return px, py, pz

    def divergence(px, py, pz, pz_before):
        bx = [pltpu.roll(px[J - 1], ye, 1)] + px[:-1]
        out = []
        for j in range(J):
            by = pltpu.roll(py[j], 1, 1)
            bz = pltpu.roll(jnp.where(row == ROWS - 1, pz_before[j], pz[j]), 1, 0)
            out.append(((px[j] - bx[j]) + (py[j] - by)) + (pz[j] - bz))
        return out

    nothing = jnp.zeros((ROWS, LANES), jnp.float32)

    def first(i, carry):
        lab, prev, acc = carry
        ahead = start_labels(jnp.minimum(i + 1, tiles - 1))
        mzi = mz(i)
        here = pl.ds(pl.multiple_of(i * ROWS, ROWS), ROWS)
        own_rows = jnp.where((i > 0) & (i < tiles - 1), 1.0, 0.0)
        u = [[] for j in range(J)]
        new_prev = []
        v = [vtile(j, i) for j in range(J)]
        w = [pull(v[j]) for j in range(J)]
        for l in range(how_many):
            s = [lab[j][l] for j in range(J)]
            px, py, pz = dual_step(s, [ahead[j][l] for j in range(J)], None, mzi)
            div = divergence(px, py, pz, prev[l])
            for j in range(J):
                p_ref[0, l, j, here, :] = px[j]
                p_ref[1, l, j, here, :] = py[j]
                p_ref[2, l, j, here, :] = pz[j]
                u[j].append(s[j] + (div[j] + w[j][l]))
            new_prev.append(pz)
        acc = list(acc)
        for j in range(J):
            new = project_simplex(u[j])
            m = mine[j] * own_rows
            vm = v[j] * m
            for l in range(how_many):
                l1_ref[l, j, here, :] = new[l]
                s1_ref[l, j, here, :] = 2.0 * new[l] - lab[j][l]
                acc[l] = acc[l] + new[l] * m
                acc[how_many + l] = acc[how_many + l] + new[l] * vm
        return ahead, new_prev, acc

    no_prev = [[nothing] * J for l in range(how_many)]
    one, two = start_labels(1), start_labels(2)
    prev = [dual_step([one[j][l] for j in range(J)], [two[j][l] for j in range(J)], None, mz(1))[2]
            for l in range(how_many)]
    _, _, acc = carry = lax.fori_loop(2, tiles - 2, first, (two, prev, [nothing] * (2 * how_many)))

    @pl.when(gz > 0)
    def _():
        z_copy(True).wait_recv()

    @pl.when(gz < Z - 1)
    def _():
        z_copy(False).wait_recv()

    _, _, acc = lax.fori_loop(tiles - 2, tiles, first, (start_labels(tiles - 2), carry[1], acc))
    _, _, acc = lax.fori_loop(0, 2, first, (start_labels(0), no_prev, acc))

    N = X * G * Z
    me = me_plane * Z + gz
    xs = [lax.rem(gx + d, X) for d in range(X)]
    gs = [lax.rem(gy + d, G) for d in range(G)]
    zs = [lax.rem(gz + d, Z) for d in range(Z)]
    offsets = [(a, b, c) for a in range(X) for b in range(G) for c in range(Z)][:0:-1]

    def reduce_start(k, acc):
        t = jnp.concatenate([jnp.sum(a, axis=0, keepdims=True) for a in acc], axis=0)
        t = jnp.where(row == lane, jnp.sum(t, axis=1, keepdims=True), 0.0)
        t = jnp.sum(t, axis=0, keepdims=True)
        sum_src[k] = t
        sum_all[k, me] = t
        for a, b, c in offsets:
            pltpu.make_async_remote_copy(
                sum_src.at[k], sum_all.at[k, me], a_send.at[k], a_recv.at[k],
                device_id={"gx": xs[a], "gy": gs[b], "gz": zs[c]}, device_id_type=MESH).start()

    def every(k):
        part = sum_all.at[k, pl.ds(0, N - 1)]
        return pltpu.make_async_remote_copy(
            part, part, a_send.at[k], a_recv.at[k],
            device_id={"gx": xs[-1], "gy": gs[-1], "gz": zs[-1]}, device_id_type=MESH)

    def reduce_finish(k):
        every(k).wait_recv()
        terms = [sum_all[k, q] for q in range(N)]
        while len(terms) > 1:
            terms = [sum(terms[q:q + 2][1:], terms[q]) for q in range(0, len(terms), 2)]
        total = terms[0]
        start = jnp.zeros((1, LANES), jnp.float32)
        for l in range(how_many):
            start = jnp.where(lane[:1] == l, PRIOR * base[l], start)
        return (pltpu.roll(total, LANES - how_many, 1) + start) / (total + PRIOR)

    reduce_start(0, acc)

    def second(i, prev):
        mzi = mz(i)
        here = pl.ds(pl.multiple_of(i * ROWS, ROWS), ROWS)
        new_prev = []
        for l in range(how_many):
            s = [at(s1_ref, l, j, i) for j in range(J)]
            sn = [at(s1_ref, l, j, i + 1) for j in range(J)]
            before = [[p_ref[k, l, j, here, :] for j in range(J)] for k in range(3)]
            px, py, pz = dual_step(s, sn, before, mzi)
            div = divergence(px, py, pz, prev[l])
            for j in range(J):
                l1_ref[l, j, here, :] = l1_ref[l, j, here, :] + div[j]
            new_prev.append(pz)
        return new_prev

    lax.fori_loop(0, tiles - 1, second, no_prev)

    centers = reduce_finish(0)
    centers = [jnp.broadcast_to(centers[:, l:l + 1], (ROWS, LANES)) for l in range(how_many)]
    cen_a = [2.0 * TAU * c for c in centers]
    cen_b = [TAU * c * c for c in centers]

    def third(i, acc):
        acc = list(acc)
        there = pl.ds(pl.multiple_of((i - 1) * ROWS, ROWS), ROWS)
        for j in range(J):
            v = vtile(j, i)
            new = project_simplex([at(l1_ref, l, j, i) + (cen_a[l] * v - cen_b[l]) for l in range(how_many)])
            vm = v * mine[j]
            for l in range(how_many):
                l2_ref[l, j, there, :] = new[l]
                acc[l] = acc[l] + new[l] * mine[j]
                acc[how_many + l] = acc[how_many + l] + new[l] * vm
        return acc

    acc = lax.fori_loop(1, tiles - 1, third, [nothing] * (2 * how_many))
    reduce_start(1, acc)

    for l in range(how_many):
        for j in range(J):
            rows[j] = l2_ref[l, j].T
            for i in range(-(-(xe - j) // J)):
                x = i * J + j - HALO
                if 0 <= x < lx:
                    lab_ref[l, x] = rows[j, i * ye + HALO:i * ye + HALO + ly, :]

    centers = reduce_finish(1)
    cen_ref[...] = centers[0, :how_many]
    for c in sends:
        c.wait_send()
    every(0).wait_send()
    every(1).wait_send()

    @pl.when(send_up)
    def _():
        for g in range(G):
            halo(True, g).wait_send()

    @pl.when(send_down)
    def _():
        for g in range(G):
            halo(False, g).wait_send()

    @pl.when(gz < Z - 1)
    def _():
        z_copy(True).wait_send()

    @pl.when(gz > 0)
    def _():
        z_copy(False).wait_send()


def solution(mesh):
    X, G, Z = mesh.shape["gx"], mesh.shape["gy"], mesh.shape["gz"]

    def local(volume, levels):
        T, ny, lz = volume.shape
        nx, nz = T * X * G, lz * Z
        lx, ly = T * G, ny // G
        ye, xe = ly + 2 * HALO, lx + 2 * HALO
        J = -(-xe // (LANES // ye))
        win = min(ny, ly + 16)
        n = levels.shape[0]
        f32 = jnp.float32
        dma = pltpu.SemaphoreType.DMA
        zrows = lz + 2 * ROWS
        return pl.pallas_call(
            functools.partial(kernel, (nx, ny, nz, G, X, Z, T)),
            out_shape=(jax.ShapeDtypeStruct((n, lx, ly, lz), f32), jax.ShapeDtypeStruct((n,), f32)),
            in_specs=[pl.BlockSpec(memory_space=pl.ANY), pl.BlockSpec(memory_space=pl.ANY)],
            out_specs=(pl.BlockSpec(memory_space=pltpu.VMEM), pl.BlockSpec(memory_space=pltpu.VMEM)),
            scratch_shapes=[
                pltpu.VMEM((T, ny, lz), f32),
                pltpu.VMEM((xe, win + 16, lz), f32),
                pltpu.VMEM((J, LANES, LANES), f32),
                pltpu.VMEM((J, zrows, LANES), f32),
                pltpu.VMEM((n, J, zrows, LANES), f32),
                pltpu.VMEM((n, J, zrows, LANES), f32),
                pltpu.VMEM((3, n, J, zrows, LANES), f32),
                pltpu.VMEM((n, J, lz, LANES), f32),
                pltpu.SMEM((n,), jnp.int32),
                pltpu.VMEM((2, 1, LANES), f32),
                pltpu.VMEM((2, X * G * Z, 1, LANES), f32),
                dma, dma, dma((G,)), dma((G,)), dma((2, G)), dma((2,)), dma((2,)), dma((2,)),
                dma((2,)), dma((2,)), dma, pltpu.SemaphoreType.REGULAR((2,)),
            ],
            compiler_params=pltpu.CompilerParams(collective_id=0, vmem_limit_bytes=16 << 20, has_side_effects=True),
        )(pltpu.with_memory_space_constraint(levels, pltpu.HBM), pltpu.with_memory_space_constraint(volume, pltpu.HBM))

    return jax.shard_map(
        local,
        mesh=mesh,
        in_specs=(P(("gx", "gy"), None, "gz"), P()),
        out_specs=(P(None, "gx", "gy", "gz"), P()),
        check_vma=False,
    )
```

```python
import functools

import jax
import jax.numpy as jnp
from jax import lax
from jax.experimental import pallas as pl
from jax.experimental.pallas import tpu as pltpu
from jax.sharding import PartitionSpec as P

TAU = 0.25
SIGMA = 0.25
LAMBDA = 0.5
PRIOR = 1.0
HALO = 2
ROWS = 8
LANES = 128
MESH = pl.DeviceIdType.MESH


def project_simplex(v):
    a, b, c, d = v
    hi1, lo1 = jnp.maximum(a, b), jnp.minimum(a, b)
    hi2, lo2 = jnp.maximum(c, d), jnp.minimum(c, d)
    s1, s2 = a + b, c + d
    top1 = jnp.maximum(hi1, hi2)
    top2 = jnp.maximum(hi1 + hi2, jnp.maximum(s1, s2))
    top3 = jnp.maximum(s1 + hi2, s2 + hi1)
    top4 = s1 + s2
    t = jnp.maximum(
        jnp.maximum(top1 - 1.0, top2 * 0.5 - 0.5),
        jnp.maximum(top3 * (1.0 / 3.0) - (1.0 / 3.0), top4 * 0.25 - 0.25),
    )
    return [jnp.maximum(x - t, 0.0) for x in v]


def kernel(cfg, levels_hbm, vol_ref, lab_ref, cen_ref, vin, buf, rows, volt, s1_ref, l1_ref, p_ref, l2_ref,
           levels, sum_src, sum_all, vin_sem, own_sem, x_send, x_recv, h_send, h_recv,
           z_send, z_recv, a_send, a_recv, lev_sem, far):
    nx, ny, nz, G, X, Z, T = cfg
    how_many = 4
    lx, ly, lz = T * G, ny // G, LANES
    ye = ly + 2 * HALO
    xe = lx + 2 * HALO
    J = volt.shape[0]
    win = ye
    gx, gy, gz = lax.axis_index("gx"), lax.axis_index("gy"), lax.axis_index("gz")
    tiles = lz // ROWS + 2

    load = pltpu.make_async_copy(vol_ref, vin, vin_sem)
    load.start()
    load_levels = pltpu.make_async_copy(levels_hbm, levels, lev_sem)
    load_levels.start()

    plane = X * G
    me_plane = gx * G + gy
    plane_peers = []
    for d in range(1, plane):
        q = lax.rem(me_plane + d, plane)
        plane_peers.append({"gx": q // G, "gy": lax.rem(q, G), "gz": gz})
    barrier = pltpu.get_barrier_semaphore()
    for peer in plane_peers:
        pl.semaphore_signal(barrier, inc=1, device_id=peer, device_id_type=MESH)
    above = {"gx": gx, "gy": gy, "gz": gz + 1}
    below = {"gx": gx, "gy": gy, "gz": gz - 1}
    has_above, has_below = gz < Z - 1, gz > 0

    @pl.when(has_above)
    def _():
        pl.semaphore_signal(barrier, inc=1, device_id=above, device_id_type=MESH)

    @pl.when(has_below)
    def _():
        pl.semaphore_signal(barrier, inc=1, device_id=below, device_id_type=MESH)

    pl.semaphore_wait(barrier, plane - 1 + has_above.astype(jnp.int32) + has_below.astype(jnp.int32))
    load.wait()

    def window(g):
        start = jnp.clip(g * ly - HALO, 0, ny - win)
        return start, start - (g * ly - 2 * HALO)

    sends = []
    for d in range(1, G):
        g = lax.rem(gy + d, G)
        src, dst = window(g)
        c = pltpu.make_async_remote_copy(
            vin.at[:, pl.ds(src, win)], buf.at[pl.ds(HALO + gy * T, T), pl.ds(dst, win)],
            x_send.at[d], x_recv.at[gy], device_id={"gx": gx, "gy": g, "gz": gz}, device_id_type=MESH)
        c.start()
        sends.append(c)

    def halo(up, g):
        src, dst = window(g)
        return pltpu.make_async_remote_copy(
            vin.at[pl.ds(T - HALO if up else 0, HALO), pl.ds(src, win)],
            buf.at[pl.ds(0 if up else HALO + lx, HALO), pl.ds(dst, win)],
            h_send.at[int(up), g], h_recv.at[int(up)],
            device_id={"gx": gx + 1 if up else gx - 1, "gy": g, "gz": gz}, device_id_type=MESH)

    send_up = (gy == G - 1) & (gx < X - 1)
    send_down = (gy == 0) & (gx > 0)

    @pl.when(send_up)
    def _():
        for g in range(G):
            halo(True, g).start()

    @pl.when(send_down)
    def _():
        for g in range(G):
            halo(False, g).start()

    upper = gz >= Z // 2

    @pl.when(has_below & jnp.logical_not(has_above))
    def _():
        pl.semaphore_signal(far.at[0], inc=1, device_id=below, device_id_type=MESH)

    @pl.when(has_above & jnp.logical_not(has_below))
    def _():
        pl.semaphore_signal(far.at[1], inc=1, device_id=above, device_id_type=MESH)

    def pass_on(down, up):
        @pl.when(down)
        def _():
            pl.semaphore_wait(far.at[0], 1)
            pl.semaphore_signal(far.at[0], inc=1, device_id=below, device_id_type=MESH)

        @pl.when(up)
        def _():
            pl.semaphore_wait(far.at[1], 1)
            pl.semaphore_signal(far.at[1], inc=1, device_id=above, device_id_type=MESH)

    src, dst = window(gy)
    own = pltpu.make_async_copy(
        vin.at[:, pl.ds(src, win)], buf.at[pl.ds(HALO + gy * T, T), pl.ds(dst, win)], own_sem)
    own.start()

    load_levels.wait()
    base = [levels[l].astype(jnp.float32) * (1.0 / 255.0) for l in range(how_many)]
    row = lax.broadcasted_iota(jnp.int32, (ROWS, LANES), 0)
    lane = lax.broadcasted_iota(jnp.int32, (ROWS, LANES), 1)
    part, yloc = lane // ye, lane % ye
    x0, y0, z0 = gx * lx - HALO, gy * ly - HALO, gz * lz
    yg = y0 + yloc
    step = TAU * SIGMA
    my = jnp.where((yg >= 0) & (yg < ny - 1), step, 0.0)
    mx, inside, mine = [], [], []
    for j in range(J):
        xloc = part * J + j
        xg = x0 + xloc
        mx.append(jnp.where((xg >= 0) & (xg < nx - 1), step, 0.0))
        inside.append((xg >= 0) & (xg < nx) & (yg >= 0) & (yg < ny) & (xloc < xe))
        mine.append(jnp.where((xloc >= HALO) & (xloc < HALO + lx) & (yloc >= HALO) & (yloc < HALO + ly), 1.0, 0.0))

    def mz(i):
        zg = z0 + (i - 1) * ROWS + row
        return jnp.where((zg >= 0) & (zg < nz - 1), step, 0.0)

    own.wait()
    for d in range(1, G):
        g = lax.rem(gy + d, G)
        pltpu.make_async_remote_copy(
            vin.at[:, pl.ds(src, win)], buf.at[pl.ds(HALO + g * T, T), pl.ds(dst, win)],
            x_send.at[d], x_recv.at[g], device_id={"gx": gx, "gy": g, "gz": gz}, device_id_type=MESH).wait_recv()

    def halo_in(up):
        return pltpu.make_async_remote_copy(
            vin.at[pl.ds(0, HALO), pl.ds(src, win)],
            buf.at[pl.ds(0 if up else HALO + lx, HALO), pl.ds(dst, win)],
            h_send.at[int(up), 0], h_recv.at[int(up)],
            device_id={"gx": gx, "gy": lax.rem(gy + 1, G), "gz": gz}, device_id_type=MESH)

    @pl.when(gx > 0)
    def _():
        halo_in(True).wait_recv()

    @pl.when(gx < X - 1)
    def _():
        halo_in(False).wait_recv()

    inner = has_above & has_below
    pass_on(upper & inner, jnp.logical_not(upper) & inner)

    for j in range(J):
        rows[j] = jnp.zeros((LANES, LANES), jnp.float32)
        for i in range(-(-(xe - j) // J)):
            rows[j, i * ye:(i + 1) * ye, :] = buf[i * J + j, HALO:HALO + ye].reshape(ye, LANES)
    for j in range(J):
        t = rows[j].T
        keep = jnp.broadcast_to(inside[j][:1], (LANES, LANES))
        volt[j, ROWS:ROWS + lz, :] = jnp.where(keep, t, 0.0)

    def z_copy(up):
        return pltpu.make_async_remote_copy(
            volt.at[:, pl.ds(lz if up else ROWS, ROWS), :],
            volt.at[:, pl.ds(0 if up else ROWS + lz, ROWS), :],
            z_send.at[int(up)], z_recv.at[int(up)],
            device_id={"gx": gx, "gy": gy, "gz": gz + 1 if up else gz - 1}, device_id_type=MESH)

    zero = jnp.zeros((J, ROWS, LANES), jnp.float32)

    @pl.when(gz < Z - 1)
    def _():
        z_copy(True).start()

    @pl.when(gz > 0)
    def _():
        z_copy(False).start()

    @pl.when(gz == 0)
    def _():
        volt[:, 0:ROWS, :] = zero

    @pl.when(gz == Z - 1)
    def _():
        volt[:, ROWS + lz:, :] = zero

    def at(ref, l, j, i):
        return ref[l, j, pl.ds(pl.multiple_of(i * ROWS, ROWS), ROWS), :]

    def vtile(j, i):
        return volt[j, pl.ds(pl.multiple_of(i * ROWS, ROWS), ROWS), :]

    base_a = [2.0 * TAU * b for b in base]
    base_b = [TAU * b * b for b in base]

    def pull(v):
        return [base_a[l] * v - base_b[l] for l in range(how_many)]

    def start_labels(i):
        return [project_simplex(pull(vtile(j, i))) for j in range(J)]

    def dual_step(s, sn, before, mzi):
        sz = [pltpu.roll(jnp.where(row == 0, sn[j], s[j]), ROWS - 1, 0) for j in range(J)]
        sy = [pltpu.roll(s[j], LANES - 1, 1) for j in range(J)]
        sx = s[1:] + [pltpu.roll(s[0], LANES - ye, 1)]
        px, py, pz = [], [], []
        for j in range(J):
            ax, ay, az = mx[j] * (sx[j] - s[j]), my * (sy[j] - s[j]), mzi * (sz[j] - s[j])
            if before is not None:
                ax, ay, az = ax + before[0][j], ay + before[1][j], az + before[2][j]
            shrink = jnp.minimum(1.0, (TAU * LAMBDA) * lax.rsqrt(ax * ax + ay * ay + az * az))
            px.append(ax * shrink)
            py.append(ay * shrink)
            pz.append(az * shrink)
        return px, py, pz

    def divergence(px, py, pz, pz_before):
        bx = [pltpu.roll(px[J - 1], ye, 1)] + px[:-1]
        out = []
        for j in range(J):
            by = pltpu.roll(py[j], 1, 1)
            bz = pltpu.roll(jnp.where(row == ROWS - 1, pz_before[j], pz[j]), 1, 0)
            out.append(((px[j] - bx[j]) + (py[j] - by)) + (pz[j] - bz))
        return out

    nothing = jnp.zeros((ROWS, LANES), jnp.float32)

    def first(i, carry):
        lab, prev, acc = carry
        ahead = start_labels(jnp.minimum(i + 1, tiles - 1))
        mzi = mz(i)
        here = pl.ds(pl.multiple_of(i * ROWS, ROWS), ROWS)
        own_rows = jnp.where((i > 0) & (i < tiles - 1), 1.0, 0.0)
        u = [[] for j in range(J)]
        new_prev = []
        v = [vtile(j, i) for j in range(J)]
        w = [pull(v[j]) for j in range(J)]
        for l in range(how_many):
            s = [lab[j][l] for j in range(J)]
            px, py, pz = dual_step(s, [ahead[j][l] for j in range(J)], None, mzi)
            div = divergence(px, py, pz, prev[l])
            for j in range(J):
                p_ref[0, l, j, here, :] = px[j]
                p_ref[1, l, j, here, :] = py[j]
                p_ref[2, l, j, here, :] = pz[j]
                u[j].append(s[j] + (div[j] + w[j][l]))
            new_prev.append(pz)
        acc = list(acc)
        for j in range(J):
            new = project_simplex(u[j])
            m = mine[j] * own_rows
            vm = v[j] * m
            for l in range(how_many):
                l1_ref[l, j, here, :] = new[l]
                s1_ref[l, j, here, :] = 2.0 * new[l] - lab[j][l]
                acc[l] = acc[l] + new[l] * m
                acc[how_many + l] = acc[how_many + l] + new[l] * vm
        return ahead, new_prev, acc

    no_prev = [[nothing] * J for l in range(how_many)]
    one, two = start_labels(1), start_labels(2)
    prev = [dual_step([one[j][l] for j in range(J)], [two[j][l] for j in range(J)], None, mz(1))[2]
            for l in range(how_many)]
    middle = tiles // 2
    carry = lax.fori_loop(2, middle, first, (two, prev, [nothing] * (2 * how_many)))
    pass_on(jnp.logical_not(upper) & inner, upper & inner)
    carry = lax.fori_loop(middle, tiles - 2, first, carry)

    @pl.when(gz > 0)
    def _():
        z_copy(True).wait_recv()

    @pl.when(gz < Z - 1)
    def _():
        z_copy(False).wait_recv()

    _, _, acc = lax.fori_loop(tiles - 2, tiles, first, carry)
    _, _, acc = lax.fori_loop(0, 2, first, (start_labels(0), no_prev, acc))

    N = X * G * Z
    me = me_plane * Z + gz
    xs = [lax.rem(gx + d, X) for d in range(X)]
    gs = [lax.rem(gy + d, G) for d in range(G)]
    zs = [lax.rem(gz + d, Z) for d in range(Z)]
    offsets = [(a, b, c) for a in range(X) for b in range(G) for c in range(Z)][:0:-1]

    def reduce_start(k, acc):
        t = jnp.concatenate([jnp.sum(a, axis=0, keepdims=True) for a in acc], axis=0)
        t = jnp.where(row == lane, jnp.sum(t, axis=1, keepdims=True), 0.0)
        t = jnp.sum(t, axis=0, keepdims=True)
        sum_src[k] = t
        sum_all[k, me] = t
        for a, b, c in offsets:
            pltpu.make_async_remote_copy(
                sum_src.at[k], sum_all.at[k, me], a_send.at[k], a_recv.at[k],
                device_id={"gx": xs[a], "gy": gs[b], "gz": zs[c]}, device_id_type=MESH).start()

    def every(k):
        part = sum_all.at[k, pl.ds(0, N - 1)]
        return pltpu.make_async_remote_copy(
            part, part, a_send.at[k], a_recv.at[k],
            device_id={"gx": xs[-1], "gy": gs[-1], "gz": zs[-1]}, device_id_type=MESH)

    def reduce_finish(k):
        every(k).wait_recv()
        terms = [sum_all[k, q] for q in range(N)]
        while len(terms) > 1:
            terms = [sum(terms[q:q + 2][1:], terms[q]) for q in range(0, len(terms), 2)]
        total = terms[0]
        start = jnp.zeros((1, LANES), jnp.float32)
        for l in range(how_many):
            start = jnp.where(lane[:1] == l, PRIOR * base[l], start)
        return (pltpu.roll(total, LANES - how_many, 1) + start) / (total + PRIOR)

    @pl.when(has_above & jnp.logical_not(has_below))
    def _():
        pl.semaphore_wait(far.at[0], 1)

    @pl.when(has_below & jnp.logical_not(has_above))
    def _():
        pl.semaphore_wait(far.at[1], 1)

    reduce_start(0, acc)

    def second(i, prev):
        mzi = mz(i)
        here = pl.ds(pl.multiple_of(i * ROWS, ROWS), ROWS)
        new_prev = []
        for l in range(how_many):
            s = [at(s1_ref, l, j, i) for j in range(J)]
            sn = [at(s1_ref, l, j, i + 1) for j in range(J)]
            before = [[p_ref[k, l, j, here, :] for j in range(J)] for k in range(3)]
            px, py, pz = dual_step(s, sn, before, mzi)
            div = divergence(px, py, pz, prev[l])
            for j in range(J):
                l1_ref[l, j, here, :] = l1_ref[l, j, here, :] + div[j]
            new_prev.append(pz)
        return new_prev

    lax.fori_loop(0, tiles - 1, second, no_prev)

    centers = reduce_finish(0)
    centers = [jnp.broadcast_to(centers[:, l:l + 1], (ROWS, LANES)) for l in range(how_many)]
    cen_a = [2.0 * TAU * c for c in centers]
    cen_b = [TAU * c * c for c in centers]

    def third(i, acc):
        acc = list(acc)
        there = pl.ds(pl.multiple_of((i - 1) * ROWS, ROWS), ROWS)
        for j in range(J):
            v = vtile(j, i)
            new = project_simplex([at(l1_ref, l, j, i) + (cen_a[l] * v - cen_b[l]) for l in range(how_many)])
            vm = v * mine[j]
            for l in range(how_many):
                l2_ref[l, j, there, :] = new[l]
                acc[l] = acc[l] + new[l] * mine[j]
                acc[how_many + l] = acc[how_many + l] + new[l] * vm
        return acc

    acc = lax.fori_loop(1, tiles - 1, third, [nothing] * (2 * how_many))
    reduce_start(1, acc)

    for l in range(how_many):
        for j in range(J):
            rows[j] = l2_ref[l, j].T
            for i in range(-(-(xe - j) // J)):
                x = i * J + j - HALO
                if 0 <= x < lx:
                    lab_ref[l, x] = rows[j, i * ye + HALO:i * ye + HALO + ly, :]

    centers = reduce_finish(1)
    cen_ref[...] = centers[0, :how_many]
    for c in sends:
        c.wait_send()
    every(0).wait_send()
    every(1).wait_send()

    @pl.when(send_up)
    def _():
        for g in range(G):
            halo(True, g).wait_send()

    @pl.when(send_down)
    def _():
        for g in range(G):
            halo(False, g).wait_send()

    @pl.when(gz < Z - 1)
    def _():
        z_copy(True).wait_send()

    @pl.when(gz > 0)
    def _():
        z_copy(False).wait_send()


def solution(mesh):
    X, G, Z = mesh.shape["gx"], mesh.shape["gy"], mesh.shape["gz"]

    def local(volume, levels):
        T, ny, lz = volume.shape
        nx, nz = T * X * G, lz * Z
        lx, ly = T * G, ny // G
        ye, xe = ly + 2 * HALO, lx + 2 * HALO
        J = -(-xe // (LANES // ye))
        n = levels.shape[0]
        f32 = jnp.float32
        dma = pltpu.SemaphoreType.DMA
        zrows = lz + 2 * ROWS
        return pl.pallas_call(
            functools.partial(kernel, (nx, ny, nz, G, X, Z, T)),
            out_shape=(jax.ShapeDtypeStruct((n, lx, ly, lz), f32), jax.ShapeDtypeStruct((n,), f32)),
            in_specs=[pl.BlockSpec(memory_space=pl.ANY), pl.BlockSpec(memory_space=pl.ANY)],
            out_specs=(pl.BlockSpec(memory_space=pltpu.VMEM), pl.BlockSpec(memory_space=pltpu.VMEM)),
            scratch_shapes=[
                pltpu.VMEM((T, ny, 1, lz), f32),
                pltpu.VMEM((xe, ye + 2 * HALO, 1, lz), f32),
                pltpu.VMEM((J, LANES, LANES), f32),
                pltpu.VMEM((J, zrows, LANES), f32),
                pltpu.VMEM((n, J, zrows, LANES), f32),
                pltpu.VMEM((n, J, zrows, LANES), f32),
                pltpu.VMEM((3, n, J, zrows, LANES), f32),
                pltpu.VMEM((n, J, lz, LANES), f32),
                pltpu.SMEM((n,), jnp.int32),
                pltpu.VMEM((2, 1, LANES), f32),
                pltpu.VMEM((2, X * G * Z, 1, LANES), f32),
                dma, dma, dma((G,)), dma((G,)), dma((2, G)), dma((2,)), dma((2,)), dma((2,)),
                dma((2,)), dma((2,)), dma, pltpu.SemaphoreType.REGULAR((2,)),
            ],
            compiler_params=pltpu.CompilerParams(collective_id=0, vmem_limit_bytes=16 << 20, has_side_effects=True),
        )(pltpu.with_memory_space_constraint(levels, pltpu.HBM),
          pltpu.with_memory_space_constraint(volume.reshape(T, ny, 1, lz), pltpu.HBM))

    return jax.shard_map(
        local,
        mesh=mesh,
        in_specs=(P(("gx", "gy"), None, "gz"), P()),
        out_specs=(P(None, "gx", "gy", "gz"), P()),
        check_vma=False,
    )
```

```python
import functools

import jax
import jax.numpy as jnp
from jax import lax
from jax.experimental import pallas as pl
from jax.experimental.pallas import tpu as pltpu
from jax.sharding import PartitionSpec as P

TAU = 0.25
SIGMA = 0.25
LAMBDA = 0.5
PRIOR = 1.0
HALO = 2
ROWS = 8
LANES = 128
MESH = pl.DeviceIdType.MESH


def project_simplex(v):
    a, b, c, d = v
    hi1, lo1 = jnp.maximum(a, b), jnp.minimum(a, b)
    hi2, lo2 = jnp.maximum(c, d), jnp.minimum(c, d)
    s1, s2 = a + b, c + d
    top1 = jnp.maximum(hi1, hi2)
    top2 = jnp.maximum(hi1 + hi2, jnp.maximum(s1, s2))
    top3 = jnp.maximum(s1 + hi2, s2 + hi1)
    top4 = s1 + s2
    t = jnp.maximum(
        jnp.maximum(top1 - 1.0, top2 * 0.5 - 0.5),
        jnp.maximum(top3 * (1.0 / 3.0) - (1.0 / 3.0), top4 * 0.25 - 0.25),
    )
    return [jnp.maximum(x - t, 0.0) for x in v]


def kernel(cfg, levels_hbm, vol_ref, lab_ref, cen_ref, vin, buf, rows, volt, s1_ref, l1_ref, p_ref, l2_ref,
           levels, sum_src, sum_all, vin_sem, own_sem, x_send, x_recv, h_send, h_recv,
           z_send, z_recv, a_send, a_recv, lev_sem, far):
    nx, ny, nz, G, X, Z, T = cfg
    how_many = 4
    lx, ly, lz = T * G, ny // G, LANES
    ye = ly + 2 * HALO
    xe = lx + 2 * HALO
    J = volt.shape[0]
    win = ye
    gx, gy, gz = lax.axis_index("gx"), lax.axis_index("gy"), lax.axis_index("gz")
    tiles = lz // ROWS + 2

    load = pltpu.make_async_copy(vol_ref, vin, vin_sem)
    load.start()
    win = ye

    def window(g):
        start = jnp.clip(g * ly - HALO, 0, ny - win)
        return start, start - (g * ly - 2 * HALO)

    src, dst = window(gy)
    own = pltpu.make_async_copy(
        vol_ref.at[:, pl.ds(src, win)], buf.at[pl.ds(HALO + gy * T, T), pl.ds(dst, win)], own_sem)
    own.start()
    load_levels = pltpu.make_async_copy(levels_hbm, levels, lev_sem)
    load_levels.start()

    plane = X * G
    me_plane = gx * G + gy
    plane_peers = []
    for d in range(1, plane):
        q = lax.rem(me_plane + d, plane)
        plane_peers.append({"gx": q // G, "gy": lax.rem(q, G), "gz": gz})
    barrier = pltpu.get_barrier_semaphore()
    for peer in plane_peers:
        pl.semaphore_signal(barrier, inc=1, device_id=peer, device_id_type=MESH)
    above = {"gx": gx, "gy": gy, "gz": gz + 1}
    below = {"gx": gx, "gy": gy, "gz": gz - 1}
    has_above, has_below = gz < Z - 1, gz > 0

    @pl.when(has_above)
    def _():
        pl.semaphore_signal(barrier, inc=1, device_id=above, device_id_type=MESH)

    @pl.when(has_below)
    def _():
        pl.semaphore_signal(barrier, inc=1, device_id=below, device_id_type=MESH)

    pl.semaphore_wait(barrier, plane - 1 + has_above.astype(jnp.int32) + has_below.astype(jnp.int32))
    load.wait()

    def halo(up, g):
        src, dst = window(g)
        return pltpu.make_async_remote_copy(
            vin.at[pl.ds(T - HALO if up else 0, HALO), pl.ds(src, win)],
            buf.at[pl.ds(0 if up else HALO + lx, HALO), pl.ds(dst, win)],
            h_send.at[int(up), g], h_recv.at[int(up)],
            device_id={"gx": gx + 1 if up else gx - 1, "gy": g, "gz": gz}, device_id_type=MESH)

    send_up = (gy == G - 1) & (gx < X - 1)
    send_down = (gy == 0) & (gx > 0)

    @pl.when(send_up)
    def _():
        for g in range(G):
            halo(True, g).start()

    @pl.when(send_down)
    def _():
        for g in range(G):
            halo(False, g).start()

    sends = []
    for d in range(1, G):
        g = lax.rem(gy + d, G)
        src, dst = window(g)
        c = pltpu.make_async_remote_copy(
            vin.at[:, pl.ds(src, win)], buf.at[pl.ds(HALO + gy * T, T), pl.ds(dst, win)],
            x_send.at[d], x_recv.at[gy], device_id={"gx": gx, "gy": g, "gz": gz}, device_id_type=MESH)
        c.start()
        sends.append(c)

    upper = gz >= Z // 2

    @pl.when(has_below & jnp.logical_not(has_above))
    def _():
        pl.semaphore_signal(far.at[0], inc=1, device_id=below, device_id_type=MESH)

    @pl.when(has_above & jnp.logical_not(has_below))
    def _():
        pl.semaphore_signal(far.at[1], inc=1, device_id=above, device_id_type=MESH)

    def pass_on(down, up):
        @pl.when(down)
        def _():
            pl.semaphore_wait(far.at[0], 1)
            pl.semaphore_signal(far.at[0], inc=1, device_id=below, device_id_type=MESH)

        @pl.when(up)
        def _():
            pl.semaphore_wait(far.at[1], 1)
            pl.semaphore_signal(far.at[1], inc=1, device_id=above, device_id_type=MESH)


    load_levels.wait()
    base = [levels[l].astype(jnp.float32) * (1.0 / 255.0) for l in range(how_many)]
    row = lax.broadcasted_iota(jnp.int32, (ROWS, LANES), 0)
    lane = lax.broadcasted_iota(jnp.int32, (ROWS, LANES), 1)
    part, yloc = lane // ye, lane % ye
    x0, y0, z0 = gx * lx - HALO, gy * ly - HALO, gz * lz
    yg = y0 + yloc
    step = TAU * SIGMA
    my = jnp.where((yg >= 0) & (yg < ny - 1), step, 0.0)
    mx, inside, mine = [], [], []
    for j in range(J):
        xloc = part * J + j
        xg = x0 + xloc
        mx.append(jnp.where((xg >= 0) & (xg < nx - 1), step, 0.0))
        inside.append((xg >= 0) & (xg < nx) & (yg >= 0) & (yg < ny) & (xloc < xe))
        mine.append(jnp.where((xloc >= HALO) & (xloc < HALO + lx) & (yloc >= HALO) & (yloc < HALO + ly), 1.0, 0.0))

    def mz(i):
        zg = z0 + (i - 1) * ROWS + row
        return jnp.where((zg >= 0) & (zg < nz - 1), step, 0.0)

    own.wait()
    for d in range(1, G):
        g = lax.rem(gy + d, G)
        pltpu.make_async_remote_copy(
            vin.at[:, pl.ds(src, win)], buf.at[pl.ds(HALO + g * T, T), pl.ds(dst, win)],
            x_send.at[d], x_recv.at[g], device_id={"gx": gx, "gy": g, "gz": gz}, device_id_type=MESH).wait_recv()

    def halo_in(up):
        return pltpu.make_async_remote_copy(
            vin.at[pl.ds(0, HALO), pl.ds(src, win)],
            buf.at[pl.ds(0 if up else HALO + lx, HALO), pl.ds(dst, win)],
            h_send.at[int(up), 0], h_recv.at[int(up)],
            device_id={"gx": gx, "gy": lax.rem(gy + 1, G), "gz": gz}, device_id_type=MESH)

    @pl.when(gx > 0)
    def _():
        halo_in(True).wait_recv()

    @pl.when(gx < X - 1)
    def _():
        halo_in(False).wait_recv()

    inner = has_above & has_below
    pass_on(upper & inner, jnp.logical_not(upper) & inner)

    for j in range(J):
        rows[j] = jnp.zeros((LANES, LANES), jnp.float32)
        for i in range(-(-(xe - j) // J)):
            rows[j, i * ye:(i + 1) * ye, :] = buf[i * J + j, HALO:HALO + ye].reshape(ye, LANES)
    for j in range(J):
        t = rows[j].T
        keep = jnp.broadcast_to(inside[j][:1], (LANES, LANES))
        volt[j, ROWS:ROWS + lz, :] = jnp.where(keep, t, 0.0)

    def z_copy(up):
        return pltpu.make_async_remote_copy(
            volt.at[:, pl.ds(lz if up else ROWS, ROWS), :],
            volt.at[:, pl.ds(0 if up else ROWS + lz, ROWS), :],
            z_send.at[int(up)], z_recv.at[int(up)],
            device_id={"gx": gx, "gy": gy, "gz": gz + 1 if up else gz - 1}, device_id_type=MESH)

    zero = jnp.zeros((J, ROWS, LANES), jnp.float32)

    @pl.when(gz < Z - 1)
    def _():
        z_copy(True).start()

    @pl.when(gz > 0)
    def _():
        z_copy(False).start()

    @pl.when(gz == 0)
    def _():
        volt[:, 0:ROWS, :] = zero

    @pl.when(gz == Z - 1)
    def _():
        volt[:, ROWS + lz:, :] = zero

    def at(ref, l, j, i):
        return ref[l, j, pl.ds(pl.multiple_of(i * ROWS, ROWS), ROWS), :]

    def vtile(j, i):
        return volt[j, pl.ds(pl.multiple_of(i * ROWS, ROWS), ROWS), :]

    base_a = [2.0 * TAU * b for b in base]
    base_b = [TAU * b * b for b in base]

    def pull(v):
        return [base_a[l] * v - base_b[l] for l in range(how_many)]

    def start_labels(i):
        return [project_simplex(pull(vtile(j, i))) for j in range(J)]

    def dual_step(s, sn, before, mzi):
        sz = [pltpu.roll(jnp.where(row == 0, sn[j], s[j]), ROWS - 1, 0) for j in range(J)]
        sy = [pltpu.roll(s[j], LANES - 1, 1) for j in range(J)]
        sx = s[1:] + [pltpu.roll(s[0], LANES - ye, 1)]
        px, py, pz = [], [], []
        for j in range(J):
            ax, ay, az = mx[j] * (sx[j] - s[j]), my * (sy[j] - s[j]), mzi * (sz[j] - s[j])
            if before is not None:
                ax, ay, az = ax + before[0][j], ay + before[1][j], az + before[2][j]
            shrink = jnp.minimum(1.0, (TAU * LAMBDA) * lax.rsqrt(ax * ax + ay * ay + az * az))
            px.append(ax * shrink)
            py.append(ay * shrink)
            pz.append(az * shrink)
        return px, py, pz

    def divergence(px, py, pz, pz_before):
        bx = [pltpu.roll(px[J - 1], ye, 1)] + px[:-1]
        out = []
        for j in range(J):
            by = pltpu.roll(py[j], 1, 1)
            bz = pltpu.roll(jnp.where(row == ROWS - 1, pz_before[j], pz[j]), 1, 0)
            out.append(((px[j] - bx[j]) + (py[j] - by)) + (pz[j] - bz))
        return out

    nothing = jnp.zeros((ROWS, LANES), jnp.float32)

    def first(i, carry):
        lab, prev, acc = carry
        ahead = start_labels(jnp.minimum(i + 1, tiles - 1))
        mzi = mz(i)
        here = pl.ds(pl.multiple_of(i * ROWS, ROWS), ROWS)
        own_rows = jnp.where((i > 0) & (i < tiles - 1), 1.0, 0.0)
        u = [[] for j in range(J)]
        new_prev = []
        v = [vtile(j, i) for j in range(J)]
        w = [pull(v[j]) for j in range(J)]
        for l in range(how_many):
            s = [lab[j][l] for j in range(J)]
            px, py, pz = dual_step(s, [ahead[j][l] for j in range(J)], None, mzi)
            div = divergence(px, py, pz, prev[l])
            for j in range(J):
                p_ref[0, l, j, here, :] = px[j]
                p_ref[1, l, j, here, :] = py[j]
                p_ref[2, l, j, here, :] = pz[j]
                u[j].append(s[j] + (div[j] + w[j][l]))
            new_prev.append(pz)
        acc = list(acc)
        for j in range(J):
            new = project_simplex(u[j])
            m = mine[j] * own_rows
            vm = v[j] * m
            for l in range(how_many):
                l1_ref[l, j, here, :] = new[l]
                s1_ref[l, j, here, :] = 2.0 * new[l] - lab[j][l]
                acc[l] = acc[l] + new[l] * m
                acc[how_many + l] = acc[how_many + l] + new[l] * vm
        return ahead, new_prev, acc

    no_prev = [[nothing] * J for l in range(how_many)]
    one, two = start_labels(1), start_labels(2)
    prev = [dual_step([one[j][l] for j in range(J)], [two[j][l] for j in range(J)], None, mz(1))[2]
            for l in range(how_many)]
    middle = tiles // 2
    carry = lax.fori_loop(2, middle, first, (two, prev, [nothing] * (2 * how_many)))
    pass_on(jnp.logical_not(upper) & inner, upper & inner)
    carry = lax.fori_loop(middle, tiles - 2, first, carry)

    @pl.when(gz > 0)
    def _():
        z_copy(True).wait_recv()

    @pl.when(gz < Z - 1)
    def _():
        z_copy(False).wait_recv()

    _, _, acc = lax.fori_loop(tiles - 2, tiles, first, carry)
    _, _, acc = lax.fori_loop(0, 2, first, (start_labels(0), no_prev, acc))

    N = X * G * Z
    me = me_plane * Z + gz
    xs = [lax.rem(gx + d, X) for d in range(X)]
    gs = [lax.rem(gy + d, G) for d in range(G)]
    zs = [lax.rem(gz + d, Z) for d in range(Z)]
    offsets = [(a, b, c) for a in range(X) for b in range(G) for c in range(Z)][:0:-1]

    def reduce_start(k, acc):
        t = jnp.concatenate([jnp.sum(a, axis=0, keepdims=True) for a in acc], axis=0)
        t = jnp.where(row == lane, jnp.sum(t, axis=1, keepdims=True), 0.0)
        t = jnp.sum(t, axis=0, keepdims=True)
        sum_src[k] = t
        sum_all[k, me] = t
        for a, b, c in offsets:
            pltpu.make_async_remote_copy(
                sum_src.at[k], sum_all.at[k, me], a_send.at[k], a_recv.at[k],
                device_id={"gx": xs[a], "gy": gs[b], "gz": zs[c]}, device_id_type=MESH).start()

    def every(k):
        part = sum_all.at[k, pl.ds(0, N - 1)]
        return pltpu.make_async_remote_copy(
            part, part, a_send.at[k], a_recv.at[k],
            device_id={"gx": xs[-1], "gy": gs[-1], "gz": zs[-1]}, device_id_type=MESH)

    def reduce_finish(k):
        every(k).wait_recv()
        terms = [sum_all[k, q] for q in range(N)]
        while len(terms) > 1:
            terms = [sum(terms[q:q + 2][1:], terms[q]) for q in range(0, len(terms), 2)]
        total = terms[0]
        start = jnp.zeros((1, LANES), jnp.float32)
        for l in range(how_many):
            start = jnp.where(lane[:1] == l, PRIOR * base[l], start)
        return (pltpu.roll(total, LANES - how_many, 1) + start) / (total + PRIOR)

    @pl.when(has_above & jnp.logical_not(has_below))
    def _():
        pl.semaphore_wait(far.at[0], 1)

    @pl.when(has_below & jnp.logical_not(has_above))
    def _():
        pl.semaphore_wait(far.at[1], 1)

    reduce_start(0, acc)

    def second(i, prev):
        mzi = mz(i)
        here = pl.ds(pl.multiple_of(i * ROWS, ROWS), ROWS)
        new_prev = []
        for l in range(how_many):
            s = [at(s1_ref, l, j, i) for j in range(J)]
            sn = [at(s1_ref, l, j, i + 1) for j in range(J)]
            before = [[p_ref[k, l, j, here, :] for j in range(J)] for k in range(3)]
            px, py, pz = dual_step(s, sn, before, mzi)
            div = divergence(px, py, pz, prev[l])
            for j in range(J):
                l1_ref[l, j, here, :] = l1_ref[l, j, here, :] + div[j]
            new_prev.append(pz)
        return new_prev

    lax.fori_loop(0, tiles - 1, second, no_prev)

    centers = reduce_finish(0)
    centers = [jnp.broadcast_to(centers[:, l:l + 1], (ROWS, LANES)) for l in range(how_many)]
    cen_a = [2.0 * TAU * c for c in centers]
    cen_b = [TAU * c * c for c in centers]

    def third(i, acc):
        acc = list(acc)
        there = pl.ds(pl.multiple_of((i - 1) * ROWS, ROWS), ROWS)
        for j in range(J):
            v = vtile(j, i)
            new = project_simplex([at(l1_ref, l, j, i) + (cen_a[l] * v - cen_b[l]) for l in range(how_many)])
            vm = v * mine[j]
            for l in range(how_many):
                l2_ref[l, j, there, :] = new[l]
                acc[l] = acc[l] + new[l] * mine[j]
                acc[how_many + l] = acc[how_many + l] + new[l] * vm
        return acc

    acc = lax.fori_loop(1, tiles - 1, third, [nothing] * (2 * how_many))
    reduce_start(1, acc)

    for l in range(how_many):
        for j in range(J):
            rows[j] = l2_ref[l, j].T
            for i in range(-(-(xe - j) // J)):
                x = i * J + j - HALO
                if 0 <= x < lx:
                    lab_ref[l, x] = rows[j, i * ye + HALO:i * ye + HALO + ly, :]

    centers = reduce_finish(1)
    cen_ref[...] = centers[0, :how_many]
    for c in sends:
        c.wait_send()
    every(0).wait_send()
    every(1).wait_send()

    @pl.when(send_up)
    def _():
        for g in range(G):
            halo(True, g).wait_send()

    @pl.when(send_down)
    def _():
        for g in range(G):
            halo(False, g).wait_send()

    @pl.when(gz < Z - 1)
    def _():
        z_copy(True).wait_send()

    @pl.when(gz > 0)
    def _():
        z_copy(False).wait_send()


def solution(mesh):
    X, G, Z = mesh.shape["gx"], mesh.shape["gy"], mesh.shape["gz"]

    def local(volume, levels):
        T, ny, lz = volume.shape
        nx, nz = T * X * G, lz * Z
        lx, ly = T * G, ny // G
        ye, xe = ly + 2 * HALO, lx + 2 * HALO
        J = -(-xe // (LANES // ye))
        n = levels.shape[0]
        f32 = jnp.float32
        dma = pltpu.SemaphoreType.DMA
        zrows = lz + 2 * ROWS
        return pl.pallas_call(
            functools.partial(kernel, (nx, ny, nz, G, X, Z, T)),
            out_shape=(jax.ShapeDtypeStruct((n, lx, ly, lz), f32), jax.ShapeDtypeStruct((n,), f32)),
            in_specs=[pl.BlockSpec(memory_space=pl.ANY), pl.BlockSpec(memory_space=pl.ANY)],
            out_specs=(pl.BlockSpec(memory_space=pltpu.VMEM), pl.BlockSpec(memory_space=pltpu.VMEM)),
            scratch_shapes=[
                pltpu.VMEM((T, ny, 1, lz), f32),
                pltpu.VMEM((xe, ye + 2 * HALO, 1, lz), f32),
                pltpu.VMEM((J, LANES, LANES), f32),
                pltpu.VMEM((J, zrows, LANES), f32),
                pltpu.VMEM((n, J, zrows, LANES), f32),
                pltpu.VMEM((n, J, zrows, LANES), f32),
                pltpu.VMEM((3, n, J, zrows, LANES), f32),
                pltpu.VMEM((n, J, lz, LANES), f32),
                pltpu.SMEM((n,), jnp.int32),
                pltpu.VMEM((2, 1, LANES), f32),
                pltpu.VMEM((2, X * G * Z, 1, LANES), f32),
                dma, dma, dma((G,)), dma((G,)), dma((2, G)), dma((2,)), dma((2,)), dma((2,)),
                dma((2,)), dma((2,)), dma, pltpu.SemaphoreType.REGULAR((2,)),
            ],
            compiler_params=pltpu.CompilerParams(collective_id=0, vmem_limit_bytes=16 << 20, has_side_effects=True),
        )(pltpu.with_memory_space_constraint(levels, pltpu.HBM),
          pltpu.with_memory_space_constraint(volume.reshape(T, ny, 1, lz), pltpu.HBM))

    return jax.shard_map(
        local,
        mesh=mesh,
        in_specs=(P(("gx", "gy"), None, "gz"), P()),
        out_specs=(P(None, "gx", "gy", "gz"), P()),
        check_vma=False,
    )
```
